512 devices in a mesh: proto: 64 (over y, x, core), sample: 8 (over z).
Axes of the slice: x: 4, y: 8, z: 8, core: 2. Of those that a mesh axis runs over, the one named last changes fastest.
Arguments:
- teacher_new: bfloat16 [2048, 384], P('sample'), may hold values from -6 to 6
- queue: bfloat16 [6144, 384], P('sample'), may hold values from -6 to 6
- student: bfloat16 [2048, 384], P('sample'), may hold values from -6 to 6
- prototypes: bfloat16 [131072, 384], P('proto'), may hold values from -1 to 1
- owners: int32 [2048, 1], P('sample'), may hold values from 0 to 7; in each aligned block of 256 rows (0 to 255, 256 to 511, ...) at most 64 rows name the same one
- queue_oldest_slot: int32 [8], P('sample'), may hold values from 0 to 767
Outputs:
- new_queue: bfloat16 [6144, 384], P('sample')
- proto_grad: float32 [131072, 384], P(('proto', 'sample'))
- loss: float32 [], replicated
The draws below stay inside these ranges and needn't reach their ends.
Inputs may be any that keep to these rules, and one draw needn't show every extreme that they name: `owners`: among the rows of one device (aligned blocks of 256 rows), no owner is named more than 64 times, a bound that some block reaches.
All inputs are finite; a program needn't handle non-finite values.
Results may differ from the reference program's by a relative error of at most 0.0034.
Values may be sent and summed in bfloat16 or wider, within the bound.
No kernel may reach another device: no remote copies, remote signals or barrier semaphores. Data moves between devices by JAX's collectives and lax.ppermute only.
A program may use at most 64 MiB of HBM per device.

```python
import math
import jax
import jax.numpy as jnp
import numpy as np
from jax import lax

FEATURE_WIDTH = 384
K_DEV = 2048
NEW_DEV = 256
ITERS = 3
QUEUE_PER_INDEX = 768
CAP = 64
PROTOTYPE_COUNT = 131072
NEW_ROWS = 2048
QUEUE = 6144
TEACHERS = 8192
GRAD_SCALE = 1048576
N_PROTO = 64
N_SAMPLE = 8


group_count = 8


def cluster_centers(key):
    return jax.random.normal(jax.random.fold_in(key, 101), (group_count, FEATURE_WIDTH), jnp.float32)


def cluster_labels(key, salt, rows):
    first = jax.random.randint(jax.random.fold_in(key, salt), (rows,), 0, group_count)
    second = jax.random.randint(jax.random.fold_in(key, salt + 1), (rows,), 0, group_count)
    return jnp.minimum(first, second)


def mixed_rows(key, labels, salt, strength, rows):
    centers = jnp.take(cluster_centers(key), labels, axis=0)
    noise_key = jax.random.fold_in(key, salt)
    noise = jax.random.normal(noise_key, (rows, FEATURE_WIDTH), jnp.float32)
    return strength * centers + jnp.sqrt(1.0 - strength * strength) * noise


def teacher_rows(key, salt, rows):
    labels = cluster_labels(key, salt, rows)
    strength = 0.6
    return jnp.clip(mixed_rows(key, labels, salt + 7, strength, rows), -6.0, 6.0)


def draw_teacher_new(key, part):
    return teacher_rows(key, 202, NEW_ROWS).astype(jnp.bfloat16)


def draw_queue(key, part):
    return teacher_rows(key, 303, QUEUE).astype(jnp.bfloat16)


def draw_student(key, part):
    labels = cluster_labels(key, 202, NEW_ROWS)
    strength = 0.3
    values = mixed_rows(key, labels, 404, strength, NEW_ROWS)
    return jnp.clip(values, -6.0, 6.0).astype(jnp.bfloat16)


def draw_prototypes(key, part):
    labels = jax.random.randint(jax.random.fold_in(key, 505), (PROTOTYPE_COUNT,), 0, group_count)
    position = jnp.arange(PROTOTYPE_COUNT, dtype=jnp.float32)[:, None] / (PROTOTYPE_COUNT - 1.0)
    strength = 0.1 + 0.7 * position * position
    values = mixed_rows(key, labels, 707, strength, PROTOTYPE_COUNT) / math.sqrt(FEATURE_WIDTH)
    return jnp.clip(values, -1.0, 1.0).astype(jnp.bfloat16)


def plant(result, own_key, least, top_value):
    extent = result.shape
    place = [jax.random.randint(jax.random.fold_in(own_key, axis), (), 0, extent[axis]) for axis in range(len(extent))]
    result = result.at[tuple(place)].set(least)
    longest = extent.index(max(extent))
    place[longest] = (place[longest] + 1) % extent[longest]
    return result.at[tuple(place)].set(top_value)


def assign_block(stream_key, own, number, rows, count, top, reach, lean):
    ranking = jax.random.permutation(stream_key, count)
    heavy_load, ordinary = load_shares(count, rows * top, reach, lean, True), load_shares(count, rows * top, reach, lean, False)
    places = jnp.arange(count)

    def named(lengths, turn):
        used = int((lengths > 0).sum())
        fixed = max(1, used // 4)
        shifted = fixed + (places - fixed + turn * (used - fixed)) % max(1, count - fixed)
        return jnp.zeros((count,), jnp.int32).at[ranking[jnp.where(places < fixed, places, shifted)]].set(jnp.asarray(lengths, jnp.int32))

    lengths = jnp.where(number % 4 == 0, named(heavy_load, number // 4), named(ordinary, number - number // 4 - 1))
    mixed = jax.random.permutation(jax.random.fold_in(own, 3), count)
    giver, sink = mixed[0:count // 2 * 2:2], mixed[1:count // 2 * 2:2]
    room = jnp.minimum(lengths[giver] - 1, reach - lengths[sink]) // 2
    room = jnp.where((giver == ranking[0]) | (sink == ranking[0]) | (lengths[sink] == 0), 0, jnp.maximum(room, 0))
    shifted = jax.random.randint(jax.random.fold_in(own, 4), (count // 2,), 0, 1 << 20) % (room + 1)
    lengths = lengths.at[giver].add(-shifted).at[sink].add(shifted)
    items = jnp.searchsorted(jnp.cumsum(lengths), jnp.arange(rows * top), side="right").astype(jnp.int32)
    grid = items.reshape(top, rows).T
    grid = grid[jax.random.permutation(jax.random.fold_in(own, 1), rows)]
    turn = jax.random.randint(jax.random.fold_in(own, 2), (rows, 1), 0, top)
    return jnp.take_along_axis(grid, (jnp.arange(top)[None, :] + turn) % top, axis=1)


def load_shares(number_of, total, most, skew, full):
    loads = [(1 << 20) // math.isqrt(rank ** skew) + 1 for rank in range(1, number_of + 1)]
    largest = most if full else min(most, max(-(-total // number_of), total * loads[0] // sum(loads)))
    least = 1 if total - largest >= number_of - 1 else 0
    holding, spare = [largest] + [least] * (number_of - 1), total - largest - least * (number_of - 1)
    while spare > 0:
        free = [i for i in range(1, number_of) if holding[i] < largest] or [i for i in range(1, number_of) if holding[i] < most]
        mass, left = sum([loads[i] for i in free]), spare
        for i in free:
            extra = min(most - holding[i], max(1, left * loads[i] // mass), spare)
            holding[i] = holding[i] + extra
            spare = spare - extra
    return np.array(holding)


def setup_inputs(seed: int = 0) -> dict:
    streams_of = jax.random.split(jax.random.key(seed), 7)
    teacher_new = draw_teacher_new(jax.random.fold_in(streams_of[6], 71), 0)
    queue = draw_queue(jax.random.fold_in(streams_of[6], 71), 0)
    student = draw_student(jax.random.fold_in(streams_of[6], 71), 0)
    prototypes = draw_prototypes(jax.random.fold_in(streams_of[6], 71), 0)
    owners_keys = jax.random.split(jax.random.fold_in(streams_of[4], 1), NEW_ROWS // NEW_DEV)
    owners_turns = jax.random.permutation(jax.random.fold_in(streams_of[4], 3), NEW_ROWS // NEW_DEV)
    owners = jax.vmap(lambda own, number: assign_block(jax.random.fold_in(streams_of[4], 2), own, number, NEW_DEV, N_SAMPLE, 1, CAP, 1))(owners_keys, owners_turns).reshape((NEW_ROWS, 1))
    queue_oldest_slot = plant(jax.random.randint(streams_of[5], (N_SAMPLE,), 0, QUEUE_PER_INDEX), jax.random.fold_in(streams_of[5], 1), 0, QUEUE_PER_INDEX - 1).astype(jnp.int32)
    return {"teacher_new": teacher_new, "queue": queue, "student": student, "prototypes": prototypes, "owners": owners, "queue_oldest_slot": queue_oldest_slot}


teacher_temp = 0.07
student_temp = 0.1
epsilon = 1e-12

def unit_rows(values):
    widened = values.astype(jnp.float32)
    length = jnp.sqrt(lax.optimization_barrier(jnp.sum(widened * widened, axis=1, keepdims=True)) + epsilon)
    return (widened / length, length)

def against(left, right):
    return lax.dot_general(left, right, (((1,), (1,)), ((), ())), preferred_element_type=jnp.float32)

def reference(teacher_new, queue, student, prototypes, owners, queue_oldest_slot):
    teacher_hat = unit_rows(jnp.concatenate([teacher_new, queue], 0))[0].astype(jnp.bfloat16)
    proto_unit, proto_length = unit_rows(prototypes)
    proto_hat = proto_unit.astype(jnp.bfloat16)
    blocks = proto_hat.reshape(N_PROTO, K_DEV, FEATURE_WIDTH)
    exp_scores = lax.map(lambda block: jnp.exp(against(teacher_hat, block) / teacher_temp), blocks)
    row_scale = jnp.ones((TEACHERS,), jnp.float32)
    proto_scale = jnp.ones((N_PROTO, K_DEV), jnp.float32)
    for iteration in range(ITERS):
        column_sums = jnp.einsum('btk,t->bk', exp_scores, row_scale, precision=lax.Precision.HIGHEST)
        proto_scale = 1.0 / (PROTOTYPE_COUNT * column_sums)
        row_totals = jnp.einsum('btk,bk->t', exp_scores, proto_scale, precision=lax.Precision.HIGHEST)
        row_scale = 1.0 / (TEACHERS * row_totals)
    targets = exp_scores[:, :NEW_ROWS, :] * proto_scale[:, None, :] * row_scale[None, :NEW_ROWS, None] * TEACHERS
    student_normalized = unit_rows(student)[0].astype(jnp.bfloat16)
    logits = lax.map(lambda block: against(student_normalized, block) / student_temp, blocks)
    exp_logits = jnp.exp(logits)
    denominator = lax.optimization_barrier(jnp.sum(exp_logits, axis=(0, 2)))
    loss = (jnp.sum(jnp.log(denominator)) - jnp.sum(targets * logits)) / NEW_ROWS
    softmax_output = exp_logits / denominator[None, :, None]
    logit_gradient = (GRAD_SCALE * (softmax_output - targets) / (NEW_ROWS * student_temp)).astype(jnp.bfloat16)
    unit_gradient = jnp.einsum('plu,lr->pur', logit_gradient.astype(jnp.float32), student_normalized.astype(jnp.float32), precision=lax.Precision.HIGHEST).reshape(PROTOTYPE_COUNT, FEATURE_WIDTH)
    proto_grad = (unit_gradient - proto_unit * lax.optimization_barrier(jnp.sum(proto_unit * unit_gradient, axis=1, keepdims=True))) / proto_length
    owner_list = owners[:, 0].astype(jnp.int32)
    onehot = (owner_list[:, None] == jnp.arange(N_SAMPLE, dtype=jnp.int32)[None, :]).astype(jnp.int32)
    ranks = lax.optimization_barrier(jnp.sum((jnp.cumsum(onehot, axis=0).astype(jnp.int32) - onehot) * onehot, axis=1))
    heads = lax.optimization_barrier(jnp.sum(onehot * queue_oldest_slot.astype(jnp.int32)[None, :], axis=1))
    target_slot = owner_list * QUEUE_PER_INDEX + (heads + ranks) % QUEUE_PER_INDEX
    new_queue = queue.at[target_slot].set(teacher_new)
    return (new_queue, proto_grad, loss)
```

```python
import functools
import math

import jax
import jax.numpy as jnp
from jax import lax
from jax.experimental import pallas as pl
from jax.experimental.pallas import tpu as pltpu
from jax.sharding import Mesh
from jax.sharding import PartitionSpec as P


FEATURE_WIDTH = 384
K_DEV = 2048
NEW_DEV = 256
ITERS = 3
QUEUE_PER_INDEX = 768
PROTO = ("proto_0", "proto_1", "proto_2")
PROTO_SAMPLE = ("proto_0", "proto_1", "proto_2", "sample")
ROWS = NEW_DEV + QUEUE_PER_INDEX

teacher_temp = 0.07
student_temp = 0.1
epsilon = 1e-12
TEACHER_EXP2 = math.log2(math.e) / teacher_temp
STUDENT_EXP2 = math.log2(math.e) / student_temp
F32 = jnp.float32
BF16 = jnp.bfloat16
VMEM = pl.BlockSpec(memory_space=pltpu.VMEM)
SMEM = pl.BlockSpec(memory_space=pltpu.SMEM)
MIB = 1024 * 1024


def call(body, out_shape, args, limit, flops, scratch=(), in_specs=None):
    return pl.pallas_call(
        body,
        out_shape=out_shape,
        in_specs=in_specs or [VMEM] * len(args),
        out_specs=jax.tree.map(lambda _: VMEM, out_shape),
        scratch_shapes=list(scratch),
        compiler_params=pltpu.CompilerParams(vmem_limit_bytes=limit * MIB),
        cost_estimate=pl.CostEstimate(flops=flops, bytes_accessed=0, transcendentals=0),
    )(*args)


def shape(dims, dtype=F32):
    return jax.ShapeDtypeStruct(dims, dtype)


def unit_rows(values):
    widened = values.astype(F32)
    length = jnp.sqrt(jnp.sum(widened * widened, axis=1, keepdims=True) + epsilon)
    return widened * (1.0 / length), length


def against(left, right):
    return lax.dot_general(left, right, (((1,), (1,)), ((), ())), preferred_element_type=F32)


def lane_sums(block):
    return jnp.sum(block.T, axis=0, keepdims=True)


def along_rows(row):
    return jnp.broadcast_to(row, (128, 128)).T


def scores_body(
    place_ref, new_ref, queue_ref, student_ref, proto_ref, scores_ref, cross_ref, sums_ref, partial_ref, hat, total
):
    hat[:NEW_DEV] = unit_rows(new_ref[...])[0].astype(BF16)
    hat[NEW_DEV:ROWS] = unit_rows(queue_ref[...])[0].astype(BF16)
    hat[ROWS:] = unit_rows(student_ref[...])[0].astype(BF16)
    total[...] = jnp.zeros_like(total)

    def tile(turn, carry):
        start = pl.multiple_of(turn * 256, 256)
        rows = pl.ds(start, 256)
        proto = unit_rows(proto_ref[rows, :])[0].astype(BF16)
        column = jnp.zeros((8, 256), F32)
        for part in range(ROWS // 256):
            span = slice(part * 256, part * 256 + 256)
            scores = jnp.exp2(against(hat[span], proto) * TEACHER_EXP2)
            scores_ref[span, rows] = scores
            column += jnp.sum(scores.reshape(32, 8, 256), axis=0)
        sums_ref[:, rows] = jnp.sum(column, axis=0, keepdims=True)
        product = against(hat[ROWS:], proto)
        cross_ref[:, rows] = scores_ref[:NEW_DEV, rows] * (product * (1.0 / student_temp))
        exped = jnp.exp2(product * STUDENT_EXP2)
        total[...] += exped[:, :128] + exped[:, 128:]
        return carry

    lax.fori_loop(0, K_DEV // 256, tile, 0)
    for part in range(NEW_DEV // 128):
        span = slice(part * 128, part * 128 + 128)
        partial_ref[:, span] = lane_sums(total[span])


def weigh_columns(source_ref, row, out_ref, span, block):
    def chunk(turn):
        lanes = slice(turn * 128, turn * 128 + 128)
        return source_ref[block, lanes] * row[:, lanes]

    total = chunk(0)
    for turn in range(1, K_DEV // 128):
        total += chunk(turn)
    out_ref[:, span] = lane_sums(total)


def row_totals_body(scores_ref, weight_ref, out_ref):
    row = weight_ref[...]

    def block(turn, carry):
        start = pl.multiple_of(turn * 128, 128)
        weigh_columns(scores_ref, row, out_ref, pl.ds(start, 128), pl.ds(start, 128))
        return carry

    lax.fori_loop(0, ROWS // 128, block, 0)


def last_totals_body(scores_ref, cross_ref, weight_ref, out_ref):
    row = weight_ref[...]
    for part in range(NEW_DEV // 128):
        block = slice(part * 128, part * 128 + 128)
        weigh_columns(scores_ref, row, out_ref, block, block)
        span = slice(NEW_DEV + part * 128, NEW_DEV + part * 128 + 128)
        weigh_columns(cross_ref, row, out_ref, span, block)


def column_sums_body(scores_ref, weight_ref, out_ref, total):
    total[...] = jnp.zeros_like(total)

    def block(turn, carry):
        start = pl.multiple_of(turn * 128, 128)
        weights = along_rows(weight_ref[:, pl.ds(start, 128)])
        for chunk in range(K_DEV // 128):
            lanes = slice(chunk * 128, chunk * 128 + 128)
            part = scores_ref[pl.ds(start, 128), lanes] * weights
            total[:, lanes] += jnp.sum(part.reshape(16, 8, 128), axis=0)
        return carry

    lax.fori_loop(0, ROWS // 128, block, 0)
    out_ref[...] = jnp.sum(total[...], axis=0, keepdims=True)


def gathered_body(
    factor, place_ref, owner_ref, denominator_ref, rows_ref, queue_ref, proto_ref, column_ref,
    scores_ref, soft_ref, student_ref, unit_ref, length_ref, out_ref, chosen,
):
    n_new = rows_ref.shape[0]
    share = unit_ref.shape[0]
    first = pl.multiple_of(place_ref[0] * share, share)
    unit, length = unit_rows(proto_ref[pl.ds(first, share), :])
    unit_ref[...] = unit
    length_ref[...] = length
    proto = unit.astype(BF16)
    columns = [
        along_rows(column_ref[:, pl.ds(pl.multiple_of(first + part * 128, 128), 128)] * factor)
        for part in range(share // 128)
    ]

    def tile(turn, carry):
        start = pl.multiple_of(turn * 256, 256)
        rows = pl.ds(start, 256)
        student = unit_rows(rows_ref[rows, :FEATURE_WIDTH])[0].astype(BF16)
        student_ref[rows, :] = student
        exped = jnp.exp2(against(proto, student) * STUDENT_EXP2)
        soft_ref[:, rows] = exped * (factor / denominator_ref[:, rows])
        teacher = unit_rows(rows_ref[rows, FEATURE_WIDTH:])[0].astype(BF16)
        scores = jnp.exp2(against(proto, teacher) * TEACHER_EXP2)
        for part in range(2):
            block = slice(part * 128, part * 128 + 128)
            for side in range(2):
                lanes = pl.ds(pl.multiple_of(start + side * 128, 128), 128)
                piece = scores[block, side * 128 : side * 128 + 128]
                scores_ref[block, lanes] = piece * columns[part]
        return carry

    lax.fori_loop(0, n_new // 256, tile, 0)

    mine = place_ref[0].astype(F32)
    head = place_ref[1].astype(F32)
    size = float(QUEUE_PER_INDEX)
    earlier = lax.broadcasted_iota(jnp.int32, (128, 128), 0)
    later = lax.broadcasted_iota(jnp.int32, (128, 128), 1)
    before = jnp.where(earlier < later, 1.0, 0.0).astype(BF16)
    slots = lax.broadcasted_iota(jnp.int32, (QUEUE_PER_INDEX, 128), 0).astype(F32)
    base = jnp.zeros((1, 1), F32)
    for chunk in range(n_new // 128):
        lanes = slice(chunk * 128, chunk * 128 + 128)
        named = jnp.where(owner_ref[:, lanes] == mine, 1.0, 0.0)
        ahead = jnp.dot(
            jnp.broadcast_to(named, (16, 128)).astype(BF16), before, preferred_element_type=F32
        )[:1]
        slot = head + base + ahead
        slot = jnp.where(slot >= size, slot - size, slot)
        slot = jnp.where(named > 0.5, slot, -1.0)
        chosen[:, lanes] = jnp.where(slots == slot, 1.0, 0.0).astype(BF16)
        base += jnp.sum(named, axis=1, keepdims=True)
    got = jnp.dot(chosen[...], rows_ref[:, FEATURE_WIDTH:], preferred_element_type=F32)
    turn = lax.broadcasted_iota(jnp.int32, (QUEUE_PER_INDEX, FEATURE_WIDTH), 0).astype(F32) - head
    turn = jnp.where(turn < 0.0, turn + size, turn)
    out_ref[...] = jnp.where(turn < base, got, queue_ref[...].astype(F32)).astype(BF16)


def gradient_body(
    soft_ref, scores_ref, row_ref, student_ref, unit_ref, length_ref, out_ref, gradient
):
    n_new = soft_ref.shape[1]
    for chunk in range(n_new // 128):
        lanes = slice(chunk * 128, chunk * 128 + 128)
        target = scores_ref[:, lanes] * row_ref[:, lanes]
        gradient[:, lanes] = (soft_ref[:, lanes] - target).astype(BF16)
    unit_gradient = jnp.dot(gradient[...], student_ref[...], preferred_element_type=F32)
    unit = unit_ref[...]
    along = jnp.sum(unit * unit_gradient, axis=1, keepdims=True)
    out_ref[...] = (unit_gradient - unit * along) / length_ref[...]


def from_everyone(row, axis):
    copies = jnp.broadcast_to(row[None], (lax.axis_size(axis), *row.shape))
    return lax.all_to_all(copies, axis, split_axis=0, concat_axis=0, tiled=True)


def on_device(teacher_new, queue, student, prototypes, owners, queue_oldest_slot):
    n_sample = lax.axis_size("sample")
    n_proto = lax.axis_size(PROTO)
    protos_total = K_DEV * n_proto
    teachers_total = ROWS * n_sample
    new_total = NEW_DEV * n_sample
    share = K_DEV // n_sample
    my_index = lax.axis_index("sample")
    grad_scale = protos_total * NEW_DEV // 32

    place = jnp.stack([my_index.astype(jnp.int32), queue_oldest_slot[0].astype(jnp.int32)])

    everyone = lax.all_gather(
        jnp.concatenate([student, teacher_new], axis=1), "sample", axis=0, tiled=True
    )

    scores, cross, sums, partial = call(
        scores_body,
        (shape((ROWS, K_DEV)), shape((NEW_DEV, K_DEV)), shape((1, K_DEV)), shape((1, NEW_DEV))),
        (place, teacher_new, queue, student, prototypes),
        8,
        2 * (ROWS + NEW_DEV) * K_DEV * FEATURE_WIDTH,
        [pltpu.VMEM((ROWS + NEW_DEV, FEATURE_WIDTH), BF16), pltpu.VMEM((NEW_DEV, 128), F32)],
        in_specs=[SMEM] + [VMEM] * 4,
    )
    owner_row = owners.reshape(1, NEW_DEV).astype(F32)
    got = from_everyone(jnp.concatenate([sums, owner_row], axis=1), "sample")
    all_owners = got[:, 0, K_DEV:].reshape(1, new_total)
    proto_scale = 1.0 / jnp.sum(got[:, :, :K_DEV] * protos_total, axis=0)

    denominator = None
    all_denominators = None
    for iteration in range(ITERS - 1):
        totals = call(row_totals_body, shape((1, ROWS)), (scores, proto_scale), 4, 2 * ROWS * K_DEV)
        if iteration == 0:
            totals = jnp.concatenate([totals, partial], axis=1)
        got = from_everyone(totals, PROTO)
        if iteration == 0:
            denominator = jnp.sum(got[:, :, ROWS:], axis=0)
        row_scale = 1.0 / jnp.sum(got[:, :, :ROWS] * teachers_total, axis=0)
        sums = call(
            column_sums_body,
            shape((1, K_DEV)),
            (scores, row_scale),
            4,
            2 * ROWS * K_DEV,
            [pltpu.VMEM((8, K_DEV), F32)],
        )
        if iteration == 0:
            sums = jnp.concatenate([sums, denominator], axis=1)
        got = from_everyone(sums, "sample")
        if iteration == 0:
            all_denominators = got[:, 0, K_DEV:].reshape(1, new_total)
        proto_scale = 1.0 / jnp.sum(got[:, :, :K_DEV] * protos_total, axis=0)

    totals = call(
        last_totals_body,
        shape((1, 2 * NEW_DEV)),
        (scores, cross, proto_scale),
        4,
        4 * NEW_DEV * K_DEV,
    )
    got = from_everyone(totals, PROTO)
    row_scale = 1.0 / jnp.sum(got[:, :, :NEW_DEV], axis=0)
    cross_totals = jnp.sum(got[:, :, NEW_DEV:], axis=0)
    my_loss = jnp.sum(jnp.log(denominator) - row_scale * cross_totals, axis=1, keepdims=True)
    got = from_everyone(
        jnp.concatenate([row_scale, jnp.broadcast_to(my_loss, (1, 128))], axis=1), "sample"
    )
    all_rows = got[:, 0, :NEW_DEV].reshape(1, new_total)
    loss = jnp.sum(got[:, 0, NEW_DEV]) / new_total

    all_scores, all_soft, all_students, my_unit, my_length, new_queue = call(
        functools.partial(gathered_body, grad_scale / (new_total * student_temp)),
        (
            shape((share, new_total)),
            shape((share, new_total)),
            shape((new_total, FEATURE_WIDTH), BF16),
            shape((share, FEATURE_WIDTH)),
            shape((share, 1)),
            shape((QUEUE_PER_INDEX, FEATURE_WIDTH), BF16),
        ),
        (place, all_owners, all_denominators, everyone, queue, prototypes, proto_scale),
        12,
        4 * share * new_total * FEATURE_WIDTH,
        [pltpu.VMEM((QUEUE_PER_INDEX, new_total), BF16)],
        in_specs=[SMEM] + [VMEM] * 6,
    )
    proto_grad = call(
        gradient_body,
        shape((share, FEATURE_WIDTH)),
        (all_soft, all_scores, all_rows, all_students, my_unit, my_length),
        8,
        2 * share * new_total * FEATURE_WIDTH,
        [pltpu.VMEM((share, new_total), BF16)],
    )
    return (new_queue, proto_grad, loss)


def solution(mesh):
    split = Mesh(
        mesh.devices.reshape(8, 4, 2, mesh.shape["sample"]),
        ("proto_0", "proto_1", "proto_2", "sample"),
    )
    return jax.shard_map(
        on_device,
        mesh=split,
        in_specs=(
            P("sample", None),
            P("sample", None),
            P("sample", None),
            P(PROTO, None),
            P("sample", None),
            P("sample"),
        ),
        out_specs=(P("sample", None), P(PROTO_SAMPLE, None), P()),
        check_vma=False,
    )
```

```python
import functools
import math

import jax
import jax.numpy as jnp
from jax import lax
from jax.experimental import pallas as pl
from jax.experimental.pallas import tpu as pltpu
from jax.sharding import Mesh
from jax.sharding import PartitionSpec as P


FEATURE_WIDTH = 384
K_DEV = 2048
NEW_DEV = 256
ITERS = 3
QUEUE_PER_INDEX = 768
PROTO = ("proto_0", "proto_1", "proto_2")
PROTO_SAMPLE = ("proto_0", "proto_1", "proto_2", "sample")
ROWS = NEW_DEV + QUEUE_PER_INDEX

teacher_temp = 0.07
student_temp = 0.1
epsilon = 1e-12
TEACHER_EXP2 = math.log2(math.e) / teacher_temp
STUDENT_EXP2 = math.log2(math.e) / student_temp
F32 = jnp.float32
BF16 = jnp.bfloat16
VMEM = pl.BlockSpec(memory_space=pltpu.VMEM)
SMEM = pl.BlockSpec(memory_space=pltpu.SMEM)
HBM = pl.BlockSpec(memory_space=pltpu.HBM)
DMA = pltpu.SemaphoreType.DMA
MIB = 1024 * 1024


def call(body, out_shape, args, limit, flops, scratch=(), in_specs=None, out_specs=None):
    return pl.pallas_call(
        body,
        out_shape=out_shape,
        in_specs=in_specs or [VMEM] * len(args),
        out_specs=out_specs or jax.tree.map(lambda _: VMEM, out_shape),
        scratch_shapes=list(scratch),
        compiler_params=pltpu.CompilerParams(vmem_limit_bytes=limit * MIB),
        cost_estimate=pl.CostEstimate(flops=flops, bytes_accessed=0, transcendentals=0),
    )(*args)


def in_hbm(value):
    return pltpu.with_memory_space_constraint(value, pltpu.HBM)


def shape(dims, dtype=F32):
    return jax.ShapeDtypeStruct(dims, dtype)


def unit_rows(values):
    widened = values.astype(F32)
    length = jnp.sqrt(jnp.sum(widened * widened, axis=1, keepdims=True) + epsilon)
    return widened * (1.0 / length), length


def against(left, right):
    return lax.dot_general(left, right, (((1,), (1,)), ((), ())), preferred_element_type=F32)


def lane_sums(block):
    return jnp.sum(block.T, axis=0, keepdims=True)


def along_rows(row):
    return jnp.broadcast_to(row, (128, 128)).T


def units_body(
    place_ref, new_hbm, queue_hbm, student_hbm, hat_ref, half_hbm, raw, half, row_sems, half_sem
):
    copies = [
        pltpu.make_async_copy(student_hbm, raw.at[pl.ds(ROWS, NEW_DEV)], row_sems.at[0]),
        pltpu.make_async_copy(new_hbm, raw.at[pl.ds(0, NEW_DEV)], row_sems.at[1]),
        pltpu.make_async_copy(queue_hbm, raw.at[pl.ds(NEW_DEV, QUEUE_PER_INDEX)], row_sems.at[2]),
    ]
    for copy in copies:
        copy.start()

    def rows_hat(turn, carry):
        rows = pl.ds(pl.multiple_of(turn * 128, 128), 128)
        hat_ref[rows, :] = unit_rows(raw[rows, :])[0].astype(BF16)
        return carry

    mine = place_ref[2] * 128
    copies[0].wait()
    lax.fori_loop(ROWS // 128, (ROWS + NEW_DEV) // 128, rows_hat, 0)
    half[:128] = hat_ref[pl.ds(pl.multiple_of(ROWS + mine, 128), 128), :]
    copies[1].wait()
    half[128:] = raw[pl.ds(pl.multiple_of(mine, 128), 128), :]
    half_copy = pltpu.make_async_copy(half, half_hbm, half_sem)
    half_copy.start()
    copies[2].wait()
    lax.fori_loop(0, ROWS // 128, rows_hat, 0)
    half_copy.wait()


def scores_body(
    hat, proto_hbm, scores_ref, cross_ref, sums_ref, partial_ref, raw_proto, total, proto_sems
):
    def proto_copy(turn):
        rows = pl.ds(pl.multiple_of(turn * 256, 256), 256)
        return pltpu.make_async_copy(proto_hbm.at[rows], raw_proto.at[rows], proto_sems.at[turn])

    for turn in range(K_DEV // 256):
        proto_copy(turn).start()
    total[...] = jnp.zeros_like(total)

    def tile(turn, carry):
        start = pl.multiple_of(turn * 256, 256)
        rows = pl.ds(start, 256)
        proto_copy(turn).wait()
        proto = unit_rows(raw_proto[rows, :])[0].astype(BF16)
        column = jnp.zeros((8, 256), F32)
        for part in range(ROWS // 256):
            span = slice(part * 256, part * 256 + 256)
            scores = jnp.exp2(against(hat[span], proto) * TEACHER_EXP2)
            scores_ref[span, rows] = scores
            column += jnp.sum(scores.reshape(32, 8, 256), axis=0)
        sums_ref[:, rows] = jnp.sum(column, axis=0, keepdims=True)
        product = against(hat[ROWS:], proto)
        cross_ref[:, rows] = scores_ref[:NEW_DEV, rows] * (product * (1.0 / student_temp))
        exped = jnp.exp2(product * STUDENT_EXP2)
        total[...] += exped[:, :128] + exped[:, 128:]
        return carry

    lax.fori_loop(0, K_DEV // 256, tile, 0)
    for part in range(NEW_DEV // 128):
        span = slice(part * 128, part * 128 + 128)
        partial_ref[:, span] = lane_sums(total[span])


def weigh_columns(source_ref, row, out_ref, span, block):
    def chunk(turn):
        lanes = slice(turn * 128, turn * 128 + 128)
        return source_ref[block, lanes] * row[:, lanes]

    total = chunk(0)
    for turn in range(1, K_DEV // 128):
        total += chunk(turn)
    out_ref[:, span] = lane_sums(total)


def row_totals_body(scores_ref, weight_ref, out_ref):
    row = weight_ref[...]

    def block(turn, carry):
        start = pl.multiple_of(turn * 128, 128)
        weigh_columns(scores_ref, row, out_ref, pl.ds(start, 128), pl.ds(start, 128))
        return carry

    lax.fori_loop(0, ROWS // 128, block, 0)


def last_totals_body(scores_ref, cross_ref, weight_ref, out_ref):
    row = weight_ref[...]
    for part in range(NEW_DEV // 128):
        block = slice(part * 128, part * 128 + 128)
        weigh_columns(scores_ref, row, out_ref, block, block)
        span = slice(NEW_DEV + part * 128, NEW_DEV + part * 128 + 128)
        weigh_columns(cross_ref, row, out_ref, span, block)


def column_sums_body(scores_ref, weight_ref, out_ref, total):
    total[...] = jnp.zeros_like(total)

    def block(turn, carry):
        start = pl.multiple_of(turn * 128, 128)
        weights = along_rows(weight_ref[:, pl.ds(start, 128)])
        for chunk in range(K_DEV // 128):
            lanes = slice(chunk * 128, chunk * 128 + 128)
            part = scores_ref[pl.ds(start, 128), lanes] * weights
            total[:, lanes] += jnp.sum(part.reshape(16, 8, 128), axis=0)
        return carry

    lax.fori_loop(0, ROWS // 128, block, 0)
    out_ref[...] = jnp.sum(total[...], axis=0, keepdims=True)


def message_lanes(chunk):
    return chunk // 2, slice((chunk % 2) * 128, (chunk % 2) * 128 + 128)


def gathered_body(
    factor, place_ref, first_ref, second_ref, everyone_hbm, queue_hbm, proto_hbm, column_ref,
    scores_ref, soft_hbm, unit_ref, length_ref, out_ref,
    rows_in, proto_in, queue_in, soft, chosen, row_sems, soft_sems, proto_sem, queue_sem,
):
    n_blocks = everyone_hbm.shape[0]
    n_new = n_blocks * 128
    share = unit_ref.shape[0]
    first = pl.multiple_of(place_ref[0] * share, share)
    proto_copy = pltpu.make_async_copy(proto_hbm.at[pl.ds(first, share)], proto_in, proto_sem)
    proto_copy.start()

    def rows_copy(turn):
        blocks = pl.ds(turn * 2, 2)
        return pltpu.make_async_copy(everyone_hbm.at[blocks], rows_in.at[blocks], row_sems.at[turn])

    def soft_copy(turn):
        lanes = pl.ds(pl.multiple_of(turn * 256, 256), 256)
        return pltpu.make_async_copy(soft.at[:, lanes], soft_hbm.at[:, lanes], soft_sems.at[turn])

    for turn in range(n_blocks // 2):
        rows_copy(turn).start()
    queue_copy = pltpu.make_async_copy(queue_hbm, queue_in, queue_sem)
    queue_copy.start()
    columns = [
        along_rows(column_ref[:, pl.ds(pl.multiple_of(first + part * 128, 128), 128)] * factor)
        for part in range(share // 128)
    ]
    proto_copy.wait()
    unit, length = unit_rows(proto_in[...])
    unit_ref[...] = unit
    length_ref[...] = length
    proto = unit.astype(BF16)

    def tile(turn, carry):
        start = pl.multiple_of(turn * 256, 256)
        rows_copy(turn).wait()
        for side in range(2):
            lanes = pl.ds(pl.multiple_of(start + side * 128, 128), 128)
            exped = jnp.exp2(against(proto, rows_in[turn * 2 + side, :128, :]) * STUDENT_EXP2)
            names = slice(K_DEV + side * 128, K_DEV + side * 128 + 128)
            soft[:, lanes] = exped * (factor / second_ref[turn, :, names])
            teacher = unit_rows(rows_in[turn * 2 + side, 128:, :])[0].astype(BF16)
            scores = jnp.exp2(against(proto, teacher) * TEACHER_EXP2)
            for part in range(2):
                block = slice(part * 128, part * 128 + 128)
                scores_ref[block, lanes] = scores[block] * columns[part]
        soft_copy(turn).start()
        return carry

    lax.fori_loop(0, n_blocks // 2, tile, 0)

    mine = place_ref[0].astype(F32)
    head = place_ref[1].astype(F32)
    size = float(QUEUE_PER_INDEX)
    earlier = lax.broadcasted_iota(jnp.int32, (128, 128), 0)
    later = lax.broadcasted_iota(jnp.int32, (128, 128), 1)
    before = jnp.where(earlier < later, 1.0, 0.0).astype(BF16)
    slots = lax.broadcasted_iota(jnp.int32, (QUEUE_PER_INDEX, 128), 0).astype(F32)
    base = jnp.zeros((1, 1), F32)
    for chunk in range(n_new // 128):
        plane, lanes = message_lanes(chunk)
        names = slice(K_DEV + lanes.start, K_DEV + lanes.stop)
        named = jnp.where(first_ref[plane, :, names] == mine, 1.0, 0.0)
        ahead = jnp.dot(
            jnp.broadcast_to(named, (16, 128)).astype(BF16), before, preferred_element_type=F32
        )[:1]
        slot = head + base + ahead
        slot = jnp.where(slot >= size, slot - size, slot)
        slot = jnp.where(named > 0.5, slot, -1.0)
        chosen[:, chunk * 128 : chunk * 128 + 128] = jnp.where(slots == slot, 1.0, 0.0).astype(BF16)
        base += jnp.sum(named, axis=1, keepdims=True)
    teachers = rows_in[:, 128:, :].reshape(n_new, FEATURE_WIDTH)
    got = jnp.dot(chosen[...], teachers, preferred_element_type=F32)
    turn = lax.broadcasted_iota(jnp.int32, (QUEUE_PER_INDEX, FEATURE_WIDTH), 0).astype(F32) - head
    turn = jnp.where(turn < 0.0, turn + size, turn)
    queue_copy.wait()
    out_ref[...] = jnp.where(turn < base, got, queue_in[...].astype(F32)).astype(BF16)
    for turn in range(n_blocks // 2):
        soft_copy(turn).wait()


def rows_body(got_ref, denominator_ref, out_ref):
    totals = jnp.sum(got_ref[...], axis=0)
    row_scale = 1.0 / totals[:, :NEW_DEV]
    terms = jnp.log(denominator_ref[...]) - row_scale * totals[:, NEW_DEV:]
    loss = jnp.broadcast_to(jnp.sum(terms, axis=1, keepdims=True), (1, 128))
    message = jnp.concatenate([row_scale, loss], axis=1)
    out_ref[...] = jnp.broadcast_to(message[None], out_ref.shape)


def gradient_body(
    got_ref, scores_ref, soft_hbm, everyone_hbm, unit_ref, length_ref, out_ref, loss_ref,
    soft, student, gradient, soft_sem, student_sem,
):
    n_blocks = student.shape[0]
    n_new = n_blocks * 128
    soft_copy = pltpu.make_async_copy(soft_hbm, soft, soft_sem)
    student_copy = pltpu.make_async_copy(
        everyone_hbm.at[:, pl.ds(0, 128), :], student, student_sem
    )
    soft_copy.start()
    student_copy.start()
    loss_ref[...] = jnp.sum(got_ref[:, :, NEW_DEV : NEW_DEV + 1], axis=0) * (1.0 / n_new)
    soft_copy.wait()
    for chunk in range(n_blocks):
        plane, names = message_lanes(chunk)
        lanes = slice(chunk * 128, chunk * 128 + 128)
        target = scores_ref[:, lanes] * got_ref[plane, :, names]
        gradient[:, lanes] = (soft[:, lanes] - target).astype(BF16)
    student_copy.wait()
    students = student[...].reshape(n_new, FEATURE_WIDTH)
    unit_gradient = jnp.dot(gradient[...], students, preferred_element_type=F32)
    unit = unit_ref[...]
    along = jnp.sum(unit * unit_gradient, axis=1, keepdims=True)
    out_ref[...] = (unit_gradient - unit * along) / length_ref[...]


def from_everyone(row, axis):
    copies = jnp.broadcast_to(row[None], (lax.axis_size(axis), *row.shape))
    return lax.all_to_all(copies, axis, split_axis=0, concat_axis=0, tiled=True)


def on_device(teacher_new, queue, student, prototypes, owners, queue_oldest_slot):
    n_sample = lax.axis_size("sample")
    n_proto = lax.axis_size(PROTO)
    protos_total = K_DEV * n_proto
    teachers_total = ROWS * n_sample
    new_total = NEW_DEV * n_sample
    share = K_DEV // n_sample
    my_index = lax.axis_index("sample")
    grad_scale = protos_total * NEW_DEV // 32
    factor = grad_scale / (new_total * student_temp)
    place = jnp.stack(
        [
            my_index.astype(jnp.int32),
            queue_oldest_slot[0].astype(jnp.int32),
            lax.axis_index("proto_2").astype(jnp.int32),
        ]
    )

    hat, half = call(
        units_body,
        (
            shape((ROWS + NEW_DEV, FEATURE_WIDTH), BF16),
            pltpu.HBM((NEW_DEV, FEATURE_WIDTH), BF16),
        ),
        (place, in_hbm(teacher_new), in_hbm(queue), in_hbm(student)),
        6,
        8 * (ROWS + NEW_DEV) * FEATURE_WIDTH,
        [
            pltpu.VMEM((ROWS + NEW_DEV, FEATURE_WIDTH), BF16),
            pltpu.VMEM((NEW_DEV, FEATURE_WIDTH), BF16),
            DMA((3,)),
            DMA,
        ],
        in_specs=[SMEM] + [HBM] * 3,
        out_specs=(VMEM, HBM),
    )
    everyone = lax.all_gather(half, ("sample", "proto_2"), axis=0)
    scores, cross, sums, partial = call(
        scores_body,
        (shape((ROWS, K_DEV)), shape((NEW_DEV, K_DEV)), shape((1, K_DEV)), shape((1, NEW_DEV))),
        (hat, in_hbm(prototypes)),
        8,
        2 * (ROWS + NEW_DEV) * K_DEV * FEATURE_WIDTH,
        [
            pltpu.VMEM((K_DEV, FEATURE_WIDTH), BF16),
            pltpu.VMEM((NEW_DEV, 128), F32),
            DMA((K_DEV // 256,)),
        ],
        in_specs=[VMEM, HBM],
    )
    owner_row = owners.reshape(1, NEW_DEV).astype(F32)
    first = from_everyone(jnp.concatenate([sums, owner_row], axis=1), "sample")
    proto_scale = 1.0 / jnp.sum(first[:, :, :K_DEV] * protos_total, axis=0)

    denominator = None
    second = None
    for iteration in range(ITERS - 1):
        totals = call(row_totals_body, shape((1, ROWS)), (scores, proto_scale), 4, 2 * ROWS * K_DEV)
        if iteration == 0:
            totals = jnp.concatenate([totals, partial], axis=1)
        got = from_everyone(totals, PROTO)
        if iteration == 0:
            denominator = jnp.sum(got[:, :, ROWS:], axis=0)
        row_scale = 1.0 / jnp.sum(got[:, :, :ROWS] * teachers_total, axis=0)
        sums = call(
            column_sums_body,
            shape((1, K_DEV)),
            (scores, row_scale),
            4,
            2 * ROWS * K_DEV,
            [pltpu.VMEM((8, K_DEV), F32)],
        )
        if iteration == 0:
            sums = jnp.concatenate([sums, denominator], axis=1)
        got = from_everyone(sums, "sample")
        if iteration == 0:
            second = got
        proto_scale = 1.0 / jnp.sum(got[:, :, :K_DEV] * protos_total, axis=0)

    totals = call(
        last_totals_body,
        shape((1, 2 * NEW_DEV)),
        (scores, cross, proto_scale),
        4,
        4 * NEW_DEV * K_DEV,
    )
    got = from_everyone(totals, PROTO)
    message = call(
        rows_body, shape((n_sample, 1, NEW_DEV + 128)), (got, denominator), 4, n_proto * 2 * NEW_DEV
    )
    got = lax.all_to_all(message, "sample", split_axis=0, concat_axis=0, tiled=True)

    all_scores, all_soft, my_unit, my_length, new_queue = call(
        functools.partial(gathered_body, factor),
        (
            shape((share, new_total)),
            pltpu.HBM((share, new_total), F32),
            shape((share, FEATURE_WIDTH)),
            shape((share, 1)),
            shape((QUEUE_PER_INDEX, FEATURE_WIDTH), BF16),
        ),
        (place, first, second, in_hbm(everyone), in_hbm(queue), in_hbm(prototypes), proto_scale),
        16,
        4 * share * new_total * FEATURE_WIDTH,
        [
            pltpu.VMEM(everyone.shape, BF16),
            pltpu.VMEM((share, FEATURE_WIDTH), BF16),
            pltpu.VMEM((QUEUE_PER_INDEX, FEATURE_WIDTH), BF16),
            pltpu.VMEM((share, new_total), F32),
            pltpu.VMEM((QUEUE_PER_INDEX, new_total), BF16),
            DMA((n_sample,)),
            DMA((n_sample,)),
            DMA,
            DMA,
        ],
        in_specs=[SMEM, VMEM, VMEM, HBM, HBM, HBM, VMEM],
        out_specs=(VMEM, HBM, VMEM, VMEM, VMEM),
    )
    proto_grad, loss = call(
        gradient_body,
        (shape((share, FEATURE_WIDTH)), shape((1, 1))),
        (got, all_scores, in_hbm(all_soft), in_hbm(everyone), my_unit, my_length),
        12,
        2 * share * new_total * FEATURE_WIDTH,
        [
            pltpu.VMEM((share, new_total), F32),
            pltpu.VMEM((new_total // 128, 128, FEATURE_WIDTH), BF16),
            pltpu.VMEM((share, new_total), BF16),
            DMA,
            DMA,
        ],
        in_specs=[VMEM, VMEM, HBM, HBM, VMEM, VMEM],
    )
    return (new_queue, proto_grad, loss.reshape(()))


def solution(mesh):
    split = Mesh(
        mesh.devices.reshape(8, 4, 2, mesh.shape["sample"]),
        ("proto_0", "proto_1", "proto_2", "sample"),
    )
    return jax.shard_map(
        on_device,
        mesh=split,
        in_specs=(
            P("sample", None),
            P("sample", None),
            P("sample", None),
            P(PROTO, None),
            P("sample", None),
            P("sample"),
        ),
        out_specs=(P("sample", None), P(PROTO_SAMPLE, None), P()),
        check_vma=False,
    )
```

```python
import functools
import math

import jax
import jax.numpy as jnp
from jax import lax
from jax.experimental import pallas as pl
from jax.experimental.pallas import tpu as pltpu
from jax.sharding import Mesh
from jax.sharding import PartitionSpec as P


FEATURE_WIDTH = 384
K_DEV = 2048
NEW_DEV = 256
ITERS = 3
QUEUE_PER_INDEX = 768
PROTO = ("proto_0", "proto_1", "proto_2")
PROTO_SAMPLE = ("proto_0", "proto_1", "proto_2", "sample")
ROWS = NEW_DEV + QUEUE_PER_INDEX

teacher_temp = 0.07
student_temp = 0.1
epsilon = 1e-12
TEACHER_EXP2 = math.log2(math.e) / teacher_temp
STUDENT_EXP2 = math.log2(math.e) / student_temp
F32 = jnp.float32
BF16 = jnp.bfloat16
VMEM = pl.BlockSpec(memory_space=pltpu.VMEM)
SMEM = pl.BlockSpec(memory_space=pltpu.SMEM)
HBM = pl.BlockSpec(memory_space=pltpu.HBM)
DMA = pltpu.SemaphoreType.DMA
MIB = 1024 * 1024


def call(body, out_shape, args, limit, flops, scratch=(), in_specs=None, out_specs=None):
    return pl.pallas_call(
        body,
        out_shape=out_shape,
        in_specs=in_specs or [VMEM] * len(args),
        out_specs=out_specs or jax.tree.map(lambda _: VMEM, out_shape),
        scratch_shapes=list(scratch),
        compiler_params=pltpu.CompilerParams(vmem_limit_bytes=limit * MIB),
        cost_estimate=pl.CostEstimate(flops=flops, bytes_accessed=0, transcendentals=0),
    )(*args)


def in_hbm(value):
    return pltpu.with_memory_space_constraint(value, pltpu.HBM)


def shape(dims, dtype=F32):
    return jax.ShapeDtypeStruct(dims, dtype)


def unit_rows(values):
    widened = values.astype(F32)
    length = jnp.sqrt(jnp.sum(widened * widened, axis=1, keepdims=True) + epsilon)
    return widened * (1.0 / length), length


def against(left, right):
    return lax.dot_general(left, right, (((1,), (1,)), ((), ())), preferred_element_type=F32)


def lane_sums(block):
    return jnp.sum(block.T, axis=0, keepdims=True)


def along_rows(row):
    return jnp.broadcast_to(row, (128, 128)).T


def units_body(
    place_ref, new_hbm, queue_hbm, student_hbm, hat_ref, half_hbm, raw, half, row_sems, half_sem
):
    copies = [
        pltpu.make_async_copy(student_hbm, raw.at[pl.ds(ROWS, NEW_DEV)], row_sems.at[0]),
        pltpu.make_async_copy(new_hbm, raw.at[pl.ds(0, NEW_DEV)], row_sems.at[1]),
        pltpu.make_async_copy(queue_hbm, raw.at[pl.ds(NEW_DEV, QUEUE_PER_INDEX)], row_sems.at[2]),
    ]
    for copy in copies:
        copy.start()

    def rows_hat(turn, carry):
        rows = pl.ds(pl.multiple_of(turn * 128, 128), 128)
        hat_ref[rows, :] = unit_rows(raw[rows, :])[0].astype(BF16)
        return carry

    mine = place_ref[2] * 128
    copies[0].wait()
    lax.fori_loop(ROWS // 128, (ROWS + NEW_DEV) // 128, rows_hat, 0)
    half[:128] = hat_ref[pl.ds(pl.multiple_of(ROWS + mine, 128), 128), :]
    copies[1].wait()
    half[128:] = raw[pl.ds(pl.multiple_of(mine, 128), 128), :]
    half_copy = pltpu.make_async_copy(half, half_hbm, half_sem)
    half_copy.start()
    copies[2].wait()
    lax.fori_loop(0, ROWS // 128, rows_hat, 0)
    half_copy.wait()


def scores_body(
    hat, owner_ref, proto_hbm,
    scores_ref, cross_ref, message_ref, partial_ref,
    raw_proto, product_even, product_odd, total, sums, proto_sems,
):
    def proto_copy(turn):
        rows = pl.ds(turn * 256, 256)
        return pltpu.make_async_copy(proto_hbm.at[rows], raw_proto.at[rows], proto_sems.at[turn])

    n_tiles = K_DEV // 256
    copies = [proto_copy(turn) for turn in range(n_tiles)]
    for copy in copies:
        copy.start()
    total[...] = jnp.zeros_like(total)
    sums[...] = jnp.zeros_like(sums)
    sums[K_DEV // 128 : K_DEV // 128 + 2] = owner_ref[...].astype(F32)
    buffers = (product_even, product_odd)

    def multiply(turn):
        copies[turn].wait()
        proto = unit_rows(raw_proto[turn * 256 : turn * 256 + 256])[0].astype(BF16)
        buffers[turn % 2][...] = against(hat[...], proto)

    def finish(turn):
        product = buffers[turn % 2]
        lanes = slice(turn * 256, turn * 256 + 256)
        column = jnp.zeros((8, 256), F32)
        for start in range(0, ROWS, 64):
            rows = slice(start, start + 64)
            scores = jnp.exp2(product[rows] * TEACHER_EXP2)
            scores_ref[rows, lanes] = scores
            column += jnp.sum(scores.reshape(8, 8, 256), axis=0)
            if start < NEW_DEV:
                logits = product[ROWS + start : ROWS + start + 64]
                cross_ref[rows, lanes] = scores * (logits * (1.0 / student_temp))
                exped = jnp.exp2(logits * STUDENT_EXP2)
                total[rows] += exped[:, :128] + exped[:, 128:]
        column = jnp.sum(column, axis=0, keepdims=True)
        sums[2 * turn : 2 * turn + 1] = column[:, :128]
        sums[2 * turn + 1 : 2 * turn + 2] = column[:, 128:]

    multiply(0)
    for turn in range(n_tiles):
        if turn + 1 < n_tiles:
            multiply(turn + 1)
        finish(turn)
    for part in range(NEW_DEV // 128):
        partial_ref[part : part + 1] = lane_sums(total[part * 128 : part * 128 + 128])
    message = sums[...].astype(BF16)
    for peer in range(message_ref.shape[0]):
        message_ref[peer] = message


def received(got_ref, n_rows):
    total = got_ref[0, :n_rows].astype(F32)
    for peer in range(1, got_ref.shape[0]):
        total += got_ref[peer, :n_rows].astype(F32)
    return total


def weigh_columns(source_ref, scale_ref, block):
    total = None
    for turn in range(K_DEV // 128):
        part = source_ref[block, turn * 128 : turn * 128 + 128] * scale_ref[turn : turn + 1]
        total = part if turn == 0 else total + part
    return lane_sums(total)


def row_totals_body(factor, got_ref, scores_ref, message_ref, scale, totals):
    scale[...] = 1.0 / (received(got_ref, K_DEV // 128) * factor)
    for part in range(ROWS // 128):
        block = slice(part * 128, part * 128 + 128)
        totals[part : part + 1] = weigh_columns(scores_ref, scale, block)
    message = totals[...].astype(message_ref.dtype)
    for peer in range(message_ref.shape[0]):
        message_ref[peer] = message


def last_totals_body(
    factor, got_ref, scores_ref, cross_ref, partial_ref, message_ref, scale_ref
):
    scale_ref[...] = 1.0 / (received(got_ref, K_DEV // 128) * factor)
    rows = []
    for source in (scores_ref, cross_ref):
        for part in range(NEW_DEV // 128):
            block = slice(part * 128, part * 128 + 128)
            rows.append(weigh_columns(source, scale_ref, block))
    for part in range(NEW_DEV // 128):
        rows.append(partial_ref[part : part + 1])
    message_ref[...] = jnp.broadcast_to(jnp.concatenate(rows, axis=1)[None], message_ref.shape)


def column_sums_body(factor, got_ref, scores_ref, message_ref, weights, sums):
    scale = 1.0 / (received(got_ref, ROWS // 128) * factor)
    for part in range(ROWS // 128):
        weights[part * 128 : part * 128 + 128] = along_rows(scale[part : part + 1])
    for chunk in range(K_DEV // 128):
        lanes = slice(chunk * 128, chunk * 128 + 128)
        total = jnp.zeros((8, 128), F32)
        for start in range(0, ROWS, 64):
            rows = slice(start, start + 64)
            part = scores_ref[rows, lanes] * weights[rows]
            total += jnp.sum(part.reshape(8, 8, 128), axis=0)
        sums[chunk : chunk + 1] = jnp.sum(total, axis=0, keepdims=True)
    message = sums[...].astype(message_ref.dtype)
    for peer in range(message_ref.shape[0]):
        message_ref[peer] = message


def message_lanes(chunk):
    return chunk // 2, slice((chunk % 2) * 128, (chunk % 2) * 128 + 128)


def gathered_body(
    factor, place_ref, first_ref, everyone_hbm, queue_hbm, proto_hbm, scale_ref,
    scores_ref, soft_hbm, unit_ref, length_ref, out_ref,
    rows_in, proto_in, queue_in, soft, chosen, row_sems, soft_sems, proto_sem, queue_sem,
):
    n_blocks = everyone_hbm.shape[0]
    n_new = n_blocks * 128
    share = unit_ref.shape[0]
    first = pl.multiple_of(place_ref[0] * share, share)
    proto_copy = pltpu.make_async_copy(proto_hbm.at[pl.ds(first, share)], proto_in, proto_sem)
    proto_copy.start()

    def rows_copy(turn):
        blocks = pl.ds(turn * 2, 2)
        return pltpu.make_async_copy(everyone_hbm.at[blocks], rows_in.at[blocks], row_sems.at[turn])

    def soft_copy(turn):
        lanes = pl.ds(pl.multiple_of(turn * 256, 256), 256)
        return pltpu.make_async_copy(soft.at[:, lanes], soft_hbm.at[:, lanes], soft_sems.at[turn])

    for turn in range(n_blocks // 2):
        rows_copy(turn).start()
    queue_copy = pltpu.make_async_copy(queue_hbm, queue_in, queue_sem)
    queue_copy.start()
    columns = [
        along_rows(scale_ref[pl.ds(place_ref[0] * 2 + part, 1), :] * factor)
        for part in range(share // 128)
    ]
    proto_copy.wait()
    unit, length = unit_rows(proto_in[...])
    unit_ref[...] = unit
    length_ref[...] = length
    proto = unit.astype(BF16)

    def tile(turn, carry):
        start = pl.multiple_of(turn * 256, 256)
        rows_copy(turn).wait()
        for side in range(2):
            lanes = pl.ds(pl.multiple_of(start + side * 128, 128), 128)
            exped = jnp.exp2(against(proto, rows_in[turn * 2 + side, :128, :]) * STUDENT_EXP2)
            soft[:, lanes] = exped
            teacher = unit_rows(rows_in[turn * 2 + side, 128:, :])[0].astype(BF16)
            scores = jnp.exp2(against(proto, teacher) * TEACHER_EXP2)
            for part in range(2):
                block = slice(part * 128, part * 128 + 128)
                scores_ref[block, lanes] = scores[block] * columns[part]
        soft_copy(turn).start()
        return carry

    lax.fori_loop(0, n_blocks // 2, tile, 0)

    mine = place_ref[0].astype(F32)
    head = place_ref[1].astype(F32)
    size = float(QUEUE_PER_INDEX)
    earlier = lax.broadcasted_iota(jnp.int32, (128, 128), 0)
    later = lax.broadcasted_iota(jnp.int32, (128, 128), 1)
    before = jnp.where(earlier < later, 1.0, 0.0).astype(BF16)
    slots = lax.broadcasted_iota(jnp.int32, (QUEUE_PER_INDEX, 128), 0).astype(F32)
    base = jnp.zeros((1, 1), F32)
    for chunk in range(n_new // 128):
        names = first_ref[chunk // 2, K_DEV // 128 : K_DEV // 128 + 8].astype(F32)
        named = jnp.where(names[chunk % 2 : chunk % 2 + 1] == mine, 1.0, 0.0)
        ahead = jnp.dot(
            jnp.broadcast_to(named, (16, 128)).astype(BF16), before, preferred_element_type=F32
        )[:1]
        slot = head + base + ahead
        slot = jnp.where(slot >= size, slot - size, slot)
        slot = jnp.where(named > 0.5, slot, -1.0)
        chosen[:, chunk * 128 : chunk * 128 + 128] = jnp.where(slots == slot, 1.0, 0.0).astype(BF16)
        base += jnp.sum(named, axis=1, keepdims=True)
    teachers = rows_in[:, 128:, :].reshape(n_new, FEATURE_WIDTH)
    got = jnp.dot(chosen[...], teachers, preferred_element_type=F32)
    turn = lax.broadcasted_iota(jnp.int32, (QUEUE_PER_INDEX, FEATURE_WIDTH), 0).astype(F32) - head
    turn = jnp.where(turn < 0.0, turn + size, turn)
    queue_copy.wait()
    out_ref[...] = jnp.where(turn < base, got, queue_in[...].astype(F32)).astype(BF16)
    for turn in range(n_blocks // 2):
        soft_copy(turn).wait()


def rows_body(got_ref, out_ref):
    totals = jnp.sum(got_ref[...], axis=0)
    row_scale = 1.0 / totals[:, :NEW_DEV]
    denominator = totals[:, 2 * NEW_DEV :]
    terms = jnp.log(denominator) - row_scale * totals[:, NEW_DEV : 2 * NEW_DEV]
    loss = jnp.broadcast_to(jnp.sum(terms, axis=1, keepdims=True), (1, 128))
    message = jnp.concatenate([row_scale, denominator, loss], axis=1)
    out_ref[...] = jnp.broadcast_to(message[None], out_ref.shape)


def gradient_body(
    factor, got_ref, scores_ref, soft_hbm, everyone_hbm, unit_ref, length_ref, out_ref, loss_ref,
    soft, student, gradient, soft_sems, student_sems,
):
    n_blocks = student.shape[0]
    n_new = n_blocks * 128
    n_parts = soft_sems.shape[0]
    step = n_blocks // n_parts
    soft_copies, student_copies = [], []
    for part in range(n_parts):
        lanes = pl.ds(part * step * 128, step * 128)
        soft_copies.append(
            pltpu.make_async_copy(soft_hbm.at[:, lanes], soft.at[:, lanes], soft_sems.at[part])
        )
        blocks = pl.ds(part * step, step)
        student_copies.append(
            pltpu.make_async_copy(
                everyone_hbm.at[blocks, pl.ds(0, 128), :], student.at[blocks], student_sems.at[part]
            )
        )
        soft_copies[part].start()
        student_copies[part].start()
    loss_at = 2 * NEW_DEV
    loss_ref[...] = jnp.sum(got_ref[:, :, loss_at : loss_at + 1], axis=0) * (1.0 / n_new)
    unit_gradient = None
    for part in range(n_parts):
        soft_copies[part].wait()
        for chunk in range(part * step, part * step + step):
            plane, names = message_lanes(chunk)
            others = slice(NEW_DEV + names.start, NEW_DEV + names.stop)
            lanes = slice(chunk * 128, chunk * 128 + 128)
            value = soft[:, lanes] * (factor / got_ref[plane, :, others])
            target = scores_ref[:, lanes] * got_ref[plane, :, names]
            gradient[:, lanes] = (value - target).astype(BF16)
        student_copies[part].wait()
        students = student[part * step : part * step + step].reshape(step * 128, FEATURE_WIDTH)
        piece = jnp.dot(
            gradient[:, part * step * 128 : (part + 1) * step * 128],
            students,
            preferred_element_type=F32,
        )
        unit_gradient = piece if part == 0 else unit_gradient + piece
    unit = unit_ref[...]
    along = jnp.sum(unit * unit_gradient, axis=1, keepdims=True)
    out_ref[...] = (unit_gradient - unit * along) / length_ref[...]


def exchange(message, axis):
    return lax.all_to_all(message, axis, split_axis=0, concat_axis=0, tiled=True)


def on_device(teacher_new, queue, student, prototypes, owners, queue_oldest_slot):
    n_sample = lax.axis_size("sample")
    n_proto = lax.axis_size(PROTO)
    protos_total = K_DEV * n_proto
    teachers_total = ROWS * n_sample
    new_total = NEW_DEV * n_sample
    share = K_DEV // n_sample
    my_index = lax.axis_index("sample")
    grad_scale = protos_total * NEW_DEV // 32
    factor = grad_scale / (new_total * student_temp)
    place = jnp.stack(
        [
            my_index.astype(jnp.int32),
            queue_oldest_slot[0].astype(jnp.int32),
            lax.axis_index("proto_2").astype(jnp.int32),
        ]
    )

    hat, half = call(
        units_body,
        (
            shape((ROWS + NEW_DEV, FEATURE_WIDTH), BF16),
            pltpu.HBM((NEW_DEV, FEATURE_WIDTH), BF16),
        ),
        (place, in_hbm(teacher_new), in_hbm(queue), in_hbm(student)),
        6,
        8 * (ROWS + NEW_DEV) * FEATURE_WIDTH,
        [
            pltpu.VMEM((ROWS + NEW_DEV, FEATURE_WIDTH), BF16),
            pltpu.VMEM((NEW_DEV, FEATURE_WIDTH), BF16),
            DMA((3,)),
            DMA,
        ],
        in_specs=[SMEM] + [HBM] * 3,
        out_specs=(VMEM, HBM),
    )
    everyone = lax.all_gather(half, ("sample", "proto_2"), axis=0)
    scores, cross, message, partial = call(
        scores_body,
        (
            shape((ROWS, K_DEV)),
            shape((NEW_DEV, K_DEV)),
            shape((n_sample, K_DEV // 128 + 8, 128), BF16),
            shape((NEW_DEV // 128, 128)),
        ),
        (hat, owners.reshape(NEW_DEV // 128, 128), in_hbm(prototypes)),
        10,
        2 * (ROWS + NEW_DEV) * K_DEV * FEATURE_WIDTH,
        [
            pltpu.VMEM((K_DEV, FEATURE_WIDTH), BF16),
            pltpu.VMEM((ROWS + NEW_DEV, 256), F32),
            pltpu.VMEM((ROWS + NEW_DEV, 256), F32),
            pltpu.VMEM((NEW_DEV, 128), F32),
            pltpu.VMEM((K_DEV // 128 + 8, 128), F32),
            DMA((K_DEV // 256,)),
        ],
        in_specs=[VMEM, VMEM, HBM],
    )
    first = got = exchange(message, "sample")
    for iteration in range(ITERS - 1):
        message = call(
            functools.partial(row_totals_body, protos_total),
            shape((n_proto, ROWS // 128, 128), BF16),
            (got, scores),
            4,
            2 * ROWS * K_DEV,
            [pltpu.VMEM((K_DEV // 128, 128), F32), pltpu.VMEM((ROWS // 128, 128), F32)],
        )
        got = exchange(message, PROTO)
        wide = iteration == ITERS - 2
        message = call(
            functools.partial(column_sums_body, teachers_total),
            shape((n_sample, K_DEV // 128, 128), F32 if wide else BF16),
            (got, scores),
            4,
            2 * ROWS * K_DEV,
            [pltpu.VMEM((ROWS, 128), F32), pltpu.VMEM((K_DEV // 128, 128), F32)],
        )
        got = exchange(message, "sample")

    message, proto_scale = call(
        functools.partial(last_totals_body, protos_total),
        (shape((n_proto, 1, 3 * NEW_DEV)), shape((K_DEV // 128, 128))),
        (got, scores, cross, partial),
        4,
        4 * NEW_DEV * K_DEV,
    )
    got = exchange(message, PROTO)
    message = call(
        rows_body, shape((n_sample, 1, 2 * NEW_DEV + 128)), (got,), 4, n_proto * 3 * NEW_DEV
    )
    got = exchange(message, "sample")

    all_scores, all_soft, my_unit, my_length, new_queue = call(
        functools.partial(gathered_body, factor),
        (
            shape((share, new_total)),
            pltpu.HBM((share, new_total), F32),
            shape((share, FEATURE_WIDTH)),
            shape((share, 1)),
            shape((QUEUE_PER_INDEX, FEATURE_WIDTH), BF16),
        ),
        (place, first, in_hbm(everyone), in_hbm(queue), in_hbm(prototypes), proto_scale),
        16,
        4 * share * new_total * FEATURE_WIDTH,
        [
            pltpu.VMEM(everyone.shape, BF16),
            pltpu.VMEM((share, FEATURE_WIDTH), BF16),
            pltpu.VMEM((QUEUE_PER_INDEX, FEATURE_WIDTH), BF16),
            pltpu.VMEM((share, new_total), F32),
            pltpu.VMEM((QUEUE_PER_INDEX, new_total), BF16),
            DMA((n_sample,)),
            DMA((n_sample,)),
            DMA,
            DMA,
        ],
        in_specs=[SMEM, VMEM, HBM, HBM, HBM, VMEM],
        out_specs=(VMEM, HBM, VMEM, VMEM, VMEM),
    )
    proto_grad, loss = call(
        functools.partial(gradient_body, factor),
        (shape((share, FEATURE_WIDTH)), shape((1, 1))),
        (got, all_scores, in_hbm(all_soft), in_hbm(everyone), my_unit, my_length),
        12,
        2 * share * new_total * FEATURE_WIDTH,
        [
            pltpu.VMEM((share, new_total), F32),
            pltpu.VMEM((new_total // 128, 128, FEATURE_WIDTH), BF16),
            pltpu.VMEM((share, new_total), BF16),
            DMA((4,)),
            DMA((4,)),
        ],
        in_specs=[VMEM, VMEM, HBM, HBM, VMEM, VMEM],
    )
    return (new_queue, proto_grad, loss.reshape(()))


def solution(mesh):
    split = Mesh(
        mesh.devices.reshape(8, 4, 2, mesh.shape["sample"]),
        ("proto_0", "proto_1", "proto_2", "sample"),
    )
    return jax.shard_map(
        on_device,
        mesh=split,
        in_specs=(
            P("sample", None),
            P("sample", None),
            P("sample", None),
            P(PROTO, None),
            P("sample", None),
            P("sample"),
        ),
        out_specs=(P("sample", None), P(PROTO_SAMPLE, None), P()),
        check_vma=False,
    )
```

```python
import functools
import math

import jax
import jax.numpy as jnp
from jax import lax
from jax.experimental import pallas as pl
from jax.experimental.pallas import tpu as pltpu
from jax.sharding import Mesh
from jax.sharding import PartitionSpec as P


FEATURE_WIDTH = 384
K_DEV = 2048
NEW_DEV = 256
ITERS = 3
QUEUE_PER_INDEX = 768
PROTO = ("proto_0", "proto_1", "proto_2")
PROTO_SAMPLE = ("proto_0", "proto_1", "proto_2", "sample")
ROWS = NEW_DEV + QUEUE_PER_INDEX

teacher_temp = 0.07
student_temp = 0.1
epsilon = 1e-12
TEACHER_EXP2 = math.log2(math.e) / teacher_temp
STUDENT_EXP2 = math.log2(math.e) / student_temp
F32 = jnp.float32
BF16 = jnp.bfloat16
VMEM = pl.BlockSpec(memory_space=pltpu.VMEM)
SMEM = pl.BlockSpec(memory_space=pltpu.SMEM)
HBM = pl.BlockSpec(memory_space=pltpu.HBM)
DMA = pltpu.SemaphoreType.DMA
MIB = 1024 * 1024


def call(body, out_shape, args, limit, flops, scratch=(), in_specs=None, out_specs=None):
    return pl.pallas_call(
        body,
        out_shape=out_shape,
        in_specs=in_specs or [VMEM] * len(args),
        out_specs=out_specs or jax.tree.map(lambda _: VMEM, out_shape),
        scratch_shapes=list(scratch),
        compiler_params=pltpu.CompilerParams(vmem_limit_bytes=limit * MIB),
        cost_estimate=pl.CostEstimate(flops=flops, bytes_accessed=0, transcendentals=0),
    )(*args)


def in_hbm(value):
    return pltpu.with_memory_space_constraint(value, pltpu.HBM)


def shape(dims, dtype=F32):
    return jax.ShapeDtypeStruct(dims, dtype)


def unit_rows(values):
    widened = values.astype(F32)
    length = jnp.sqrt(jnp.sum(widened * widened, axis=1, keepdims=True) + epsilon)
    return widened * (1.0 / length), length


def against(left, right):
    return lax.dot_general(left, right, (((1,), (1,)), ((), ())), preferred_element_type=F32)


def lane_sums(block):
    return jnp.sum(block.T, axis=0, keepdims=True)


def along_rows(row):
    return jnp.broadcast_to(row, (128, 128)).T


def units_body(
    place_ref, new_hbm, queue_hbm, student_hbm, hat_ref, half_hbm, raw, half, row_sems, half_sem
):
    copies = [
        pltpu.make_async_copy(student_hbm, raw.at[pl.ds(ROWS, NEW_DEV)], row_sems.at[0]),
        pltpu.make_async_copy(new_hbm, raw.at[pl.ds(0, NEW_DEV)], row_sems.at[1]),
        pltpu.make_async_copy(queue_hbm, raw.at[pl.ds(NEW_DEV, QUEUE_PER_INDEX)], row_sems.at[2]),
    ]
    for copy in copies:
        copy.start()

    def rows_hat(first, last):
        for start in range(first, last, 64):
            rows = slice(start, start + 64)
            hat_ref[rows] = unit_rows(raw[rows])[0].astype(BF16)

    mine = place_ref[2] * 128
    copies[0].wait()
    rows_hat(ROWS, ROWS + NEW_DEV)
    half[:128] = hat_ref[pl.ds(pl.multiple_of(ROWS + mine, 128), 128), :]
    copies[1].wait()
    half[128:] = raw[pl.ds(pl.multiple_of(mine, 128), 128), :]
    half_copy = pltpu.make_async_copy(half, half_hbm, half_sem)
    half_copy.start()
    rows_hat(0, NEW_DEV)
    copies[2].wait()
    rows_hat(NEW_DEV, ROWS)
    half_copy.wait()


def scores_body(
    hat, owner_hbm, proto_hbm,
    scores_ref, cross_ref, message_ref, partial_ref,
    raw_proto, proto_hat, total, sums, owner, proto_sems, owner_sem,
):
    def proto_copy(turn):
        rows = pl.ds(turn * 256, 256)
        return pltpu.make_async_copy(proto_hbm.at[rows], raw_proto.at[rows], proto_sems.at[turn])

    n_tiles = K_DEV // 256
    copies = [proto_copy(turn) for turn in range(n_tiles)]
    for copy in copies:
        copy.start()
    owner_copy = pltpu.make_async_copy(owner_hbm, owner, owner_sem)
    owner_copy.start()
    total[...] = jnp.zeros_like(total)
    sums[...] = jnp.zeros_like(sums)
    steps = [(start, min(512, ROWS - start)) for start in range(0, ROWS, 512)]

    def normalize(turn):
        copies[turn].wait()
        span = slice(turn * 256, turn * 256 + 256)
        proto_hat[turn % 2] = unit_rows(raw_proto[span])[0].astype(BF16)

    def finish(turn):
        lanes = slice(turn * 256, turn * 256 + 256)
        proto = proto_hat[turn % 2]
        column = jnp.zeros((8, 256), F32)
        for first, length in steps:
            product = against(hat[first : first + length], proto)
            for start in range(0, length, 64):
                rows = slice(first + start, first + start + 64)
                scores = jnp.exp2(product[start : start + 64] * TEACHER_EXP2)
                scores_ref[rows, lanes] = scores
                column += jnp.sum(scores.reshape(8, 8, 256), axis=0)
        product = against(hat[ROWS:], proto)
        for start in range(0, NEW_DEV, 64):
            rows = slice(start, start + 64)
            logits = product[rows]
            cross_ref[rows, lanes] = scores_ref[rows, lanes] * (logits * (1.0 / student_temp))
            exped = jnp.exp2(logits * STUDENT_EXP2)
            total[rows] += exped[:, :128] + exped[:, 128:]
        column = jnp.sum(column, axis=0, keepdims=True)
        sums[2 * turn : 2 * turn + 1] = column[:, :128]
        sums[2 * turn + 1 : 2 * turn + 2] = column[:, 128:]

    normalize(0)
    for turn in range(n_tiles):
        if turn + 1 < n_tiles:
            normalize(turn + 1)
        finish(turn)
    for part in range(NEW_DEV // 128):
        partial_ref[part : part + 1] = lane_sums(total[part * 128 : part * 128 + 128])
    owner_copy.wait()
    sums[K_DEV // 128 : K_DEV // 128 + 2] = owner[...].astype(F32)
    message = sums[...].astype(BF16)
    for peer in range(message_ref.shape[0]):
        message_ref[peer] = message


def received(got_ref, n_rows):
    total = got_ref[0, :n_rows].astype(F32)
    for peer in range(1, got_ref.shape[0]):
        total += got_ref[peer, :n_rows].astype(F32)
    return total


def weigh_columns(source_ref, scale_ref, block):
    total = None
    for turn in range(K_DEV // 128):
        part = source_ref[block, turn * 128 : turn * 128 + 128] * scale_ref[turn : turn + 1]
        total = part if turn == 0 else total + part
    return lane_sums(total)


def row_totals_body(factor, got_ref, scores_ref, message_ref, scale, totals):
    scale[...] = 1.0 / (received(got_ref, K_DEV // 128) * factor)
    for part in range(ROWS // 128):
        block = slice(part * 128, part * 128 + 128)
        totals[part : part + 1] = weigh_columns(scores_ref, scale, block)
    message = totals[...].astype(message_ref.dtype)
    for peer in range(message_ref.shape[0]):
        message_ref[peer] = message


def last_totals_body(
    factor, got_ref, scores_ref, cross_ref, partial_ref, message_ref, scale_ref
):
    scale_ref[...] = 1.0 / (received(got_ref, K_DEV // 128) * factor)
    rows = []
    for source in (scores_ref, cross_ref):
        for part in range(NEW_DEV // 128):
            block = slice(part * 128, part * 128 + 128)
            rows.append(weigh_columns(source, scale_ref, block))
    for part in range(NEW_DEV // 128):
        rows.append(partial_ref[part : part + 1])
    message_ref[...] = jnp.broadcast_to(jnp.concatenate(rows, axis=1)[None], message_ref.shape)


def column_sums_body(factor, got_ref, scores_ref, message_ref, weights, sums):
    scale = 1.0 / (received(got_ref, ROWS // 128) * factor)
    for part in range(ROWS // 128):
        weights[part * 128 : part * 128 + 128] = along_rows(scale[part : part + 1])
    for chunk in range(K_DEV // 128):
        lanes = slice(chunk * 128, chunk * 128 + 128)
        total = jnp.zeros((8, 128), F32)
        for start in range(0, ROWS, 64):
            rows = slice(start, start + 64)
            part = scores_ref[rows, lanes] * weights[rows]
            total += jnp.sum(part.reshape(8, 8, 128), axis=0)
        sums[chunk : chunk + 1] = jnp.sum(total, axis=0, keepdims=True)
    message = sums[...].astype(message_ref.dtype)
    for peer in range(message_ref.shape[0]):
        message_ref[peer] = message


def message_lanes(chunk):
    return chunk // 2, slice((chunk % 2) * 128, (chunk % 2) * 128 + 128)


def gathered_body(
    factor, place_ref, first_ref, everyone_hbm, queue_hbm, proto_hbm, scale_ref,
    scores_ref, soft_hbm, unit_ref, length_ref, out_ref,
    rows_in, proto_in, queue_in, soft, chosen, row_sems, soft_sems, proto_sem, queue_sem,
):
    n_blocks = everyone_hbm.shape[0]
    n_new = n_blocks * 128
    share = unit_ref.shape[0]
    first = pl.multiple_of(place_ref[0] * share, share)
    proto_copy = pltpu.make_async_copy(proto_hbm.at[pl.ds(first, share)], proto_in, proto_sem)
    proto_copy.start()

    def rows_copy(turn):
        blocks = pl.ds(turn * 2, 2)
        return pltpu.make_async_copy(everyone_hbm.at[blocks], rows_in.at[blocks], row_sems.at[turn])

    def soft_copy(turn):
        lanes = pl.ds(pl.multiple_of(turn * 256, 256), 256)
        return pltpu.make_async_copy(soft.at[:, lanes], soft_hbm.at[:, lanes], soft_sems.at[turn])

    for turn in range(n_blocks // 2):
        rows_copy(turn).start()
    queue_copy = pltpu.make_async_copy(queue_hbm, queue_in, queue_sem)
    queue_copy.start()
    columns = [
        along_rows(scale_ref[pl.ds(place_ref[0] * 2 + part, 1), :] * factor)
        for part in range(share // 128)
    ]
    proto_copy.wait()
    unit, length = unit_rows(proto_in[...])
    unit_ref[...] = unit
    length_ref[...] = length
    proto = unit.astype(BF16)

    def tile(turn, carry):
        start = pl.multiple_of(turn * 256, 256)
        rows_copy(turn).wait()
        for side in range(2):
            lanes = pl.ds(pl.multiple_of(start + side * 128, 128), 128)
            exped = jnp.exp2(against(proto, rows_in[turn * 2 + side, :128, :]) * STUDENT_EXP2)
            soft[:, lanes] = exped
            teacher = unit_rows(rows_in[turn * 2 + side, 128:, :])[0].astype(BF16)
            scores = jnp.exp2(against(proto, teacher) * TEACHER_EXP2)
            for part in range(2):
                block = slice(part * 128, part * 128 + 128)
                scores_ref[block, lanes] = scores[block] * columns[part]
        soft_copy(turn).start()
        return carry

    lax.fori_loop(0, n_blocks // 2, tile, 0)

    mine = place_ref[0].astype(F32)
    head = place_ref[1].astype(F32)
    size = float(QUEUE_PER_INDEX)
    earlier = lax.broadcasted_iota(jnp.int32, (128, 128), 0)
    later = lax.broadcasted_iota(jnp.int32, (128, 128), 1)
    before = jnp.where(earlier < later, 1.0, 0.0).astype(BF16)
    slots = lax.broadcasted_iota(jnp.int32, (QUEUE_PER_INDEX, 128), 0).astype(F32)
    base = jnp.zeros((1, 1), F32)
    for chunk in range(n_new // 128):
        names = first_ref[chunk // 2, K_DEV // 128 : K_DEV // 128 + 8].astype(F32)
        named = jnp.where(names[chunk % 2 : chunk % 2 + 1] == mine, 1.0, 0.0)
        ahead = jnp.dot(
            jnp.broadcast_to(named, (16, 128)).astype(BF16), before, preferred_element_type=F32
        )[:1]
        slot = head + base + ahead
        slot = jnp.where(slot >= size, slot - size, slot)
        slot = jnp.where(named > 0.5, slot, -1.0)
        chosen[:, chunk * 128 : chunk * 128 + 128] = jnp.where(slots == slot, 1.0, 0.0).astype(BF16)
        base += jnp.sum(named, axis=1, keepdims=True)
    teachers = rows_in[:, 128:, :].reshape(n_new, FEATURE_WIDTH)
    got = jnp.dot(chosen[...], teachers, preferred_element_type=F32)
    turn = lax.broadcasted_iota(jnp.int32, (QUEUE_PER_INDEX, FEATURE_WIDTH), 0).astype(F32) - head
    turn = jnp.where(turn < 0.0, turn + size, turn)
    queue_copy.wait()
    out_ref[...] = jnp.where(turn < base, got, queue_in[...].astype(F32)).astype(BF16)
    for turn in range(n_blocks // 2):
        soft_copy(turn).wait()


def rows_body(got_ref, out_ref):
    totals = jnp.sum(got_ref[...], axis=0)
    row_scale = 1.0 / totals[:, :NEW_DEV]
    denominator = totals[:, 2 * NEW_DEV :]
    terms = jnp.log(denominator) - row_scale * totals[:, NEW_DEV : 2 * NEW_DEV]
    loss = jnp.broadcast_to(jnp.sum(terms, axis=1, keepdims=True), (1, 128))
    message = jnp.concatenate([row_scale, denominator, loss], axis=1)
    out_ref[...] = jnp.broadcast_to(message[None], out_ref.shape)


def gradient_body(
    factor, got_ref, scores_ref, soft_hbm, everyone_hbm, unit_ref, length_ref, out_ref, loss_ref,
    soft, student, gradient, soft_sems, student_sems,
):
    n_blocks = student.shape[0]
    n_new = n_blocks * 128
    n_parts = soft_sems.shape[0]
    step = n_blocks // n_parts
    soft_copies, student_copies = [], []
    for part in range(n_parts):
        lanes = pl.ds(part * step * 128, step * 128)
        soft_copies.append(
            pltpu.make_async_copy(soft_hbm.at[:, lanes], soft.at[:, lanes], soft_sems.at[part])
        )
        blocks = pl.ds(part * step, step)
        student_copies.append(
            pltpu.make_async_copy(
                everyone_hbm.at[blocks, pl.ds(0, 128), :], student.at[blocks], student_sems.at[part]
            )
        )
        soft_copies[part].start()
        student_copies[part].start()
    loss_at = 2 * NEW_DEV
    loss_ref[...] = jnp.sum(got_ref[:, :, loss_at : loss_at + 1], axis=0) * (1.0 / n_new)
    for part in range(n_parts):
        soft_copies[part].wait()
        for chunk in range(part * step, part * step + step):
            plane, names = message_lanes(chunk)
            others = slice(NEW_DEV + names.start, NEW_DEV + names.stop)
            lanes = slice(chunk * 128, chunk * 128 + 128)
            value = soft[:, lanes] * (factor / got_ref[plane, :, others])
            target = scores_ref[:, lanes] * got_ref[plane, :, names]
            gradient[:, lanes] = (value - target).astype(BF16)
    for copy in student_copies:
        copy.wait()
    students = student[...].reshape(n_new, FEATURE_WIDTH)
    unit_gradient = jnp.dot(gradient[...], students, preferred_element_type=F32)
    unit = unit_ref[...]
    along = jnp.sum(unit * unit_gradient, axis=1, keepdims=True)
    out_ref[...] = (unit_gradient - unit * along) / length_ref[...]


def exchange(message, axis):
    return lax.all_to_all(message, axis, split_axis=0, concat_axis=0, tiled=True)


def on_device(teacher_new, queue, student, prototypes, owners, queue_oldest_slot):
    n_sample = lax.axis_size("sample")
    n_proto = lax.axis_size(PROTO)
    protos_total = K_DEV * n_proto
    teachers_total = ROWS * n_sample
    new_total = NEW_DEV * n_sample
    share = K_DEV // n_sample
    my_index = lax.axis_index("sample")
    grad_scale = protos_total * NEW_DEV // 32
    factor = grad_scale / (new_total * student_temp)
    place = jnp.stack(
        [
            my_index.astype(jnp.int32),
            queue_oldest_slot[0].astype(jnp.int32),
            lax.axis_index("proto_2").astype(jnp.int32),
        ]
    )

    hat, half = call(
        units_body,
        (
            shape((ROWS + NEW_DEV, FEATURE_WIDTH), BF16),
            pltpu.HBM((NEW_DEV, FEATURE_WIDTH), BF16),
        ),
        (place, in_hbm(teacher_new), in_hbm(queue), in_hbm(student)),
        6,
        8 * (ROWS + NEW_DEV) * FEATURE_WIDTH,
        [
            pltpu.VMEM((ROWS + NEW_DEV, FEATURE_WIDTH), BF16),
            pltpu.VMEM((NEW_DEV, FEATURE_WIDTH), BF16),
            DMA((3,)),
            DMA,
        ],
        in_specs=[SMEM] + [HBM] * 3,
        out_specs=(VMEM, HBM),
    )
    everyone = lax.all_gather(half, ("sample", "proto_2"), axis=0)
    scores, cross, message, partial = call(
        scores_body,
        (
            shape((ROWS, K_DEV)),
            shape((NEW_DEV, K_DEV)),
            shape((n_sample, K_DEV // 128 + 8, 128), BF16),
            shape((NEW_DEV // 128, 128)),
        ),
        (hat, in_hbm(owners.reshape(NEW_DEV // 128, 128)), in_hbm(prototypes)),
        10,
        2 * (ROWS + NEW_DEV) * K_DEV * FEATURE_WIDTH,
        [
            pltpu.VMEM((K_DEV, FEATURE_WIDTH), BF16),
            pltpu.VMEM((2, 256, FEATURE_WIDTH), BF16),
            pltpu.VMEM((NEW_DEV, 128), F32),
            pltpu.VMEM((K_DEV // 128 + 8, 128), F32),
            pltpu.VMEM((NEW_DEV // 128, 128), jnp.int32),
            DMA((K_DEV // 256,)),
            DMA,
        ],
        in_specs=[VMEM, HBM, HBM],
    )
    first = got = exchange(message, "sample")
    for iteration in range(ITERS - 1):
        message = call(
            functools.partial(row_totals_body, protos_total),
            shape((n_proto, ROWS // 128, 128), BF16),
            (got, scores),
            4,
            2 * ROWS * K_DEV,
            [pltpu.VMEM((K_DEV // 128, 128), F32), pltpu.VMEM((ROWS // 128, 128), F32)],
        )
        got = exchange(message, PROTO)
        wide = iteration == ITERS - 2
        message = call(
            functools.partial(column_sums_body, teachers_total),
            shape((n_sample, K_DEV // 128, 128), F32 if wide else BF16),
            (got, scores),
            4,
            2 * ROWS * K_DEV,
            [pltpu.VMEM((ROWS, 128), F32), pltpu.VMEM((K_DEV // 128, 128), F32)],
        )
        got = exchange(message, "sample")

    message, proto_scale = call(
        functools.partial(last_totals_body, protos_total),
        (shape((n_proto, 1, 3 * NEW_DEV)), shape((K_DEV // 128, 128))),
        (got, scores, cross, partial),
        4,
        4 * NEW_DEV * K_DEV,
    )
    got = exchange(message, PROTO)
    message = call(
        rows_body, shape((n_sample, 1, 2 * NEW_DEV + 128)), (got,), 4, n_proto * 3 * NEW_DEV
    )
    got = exchange(message, "sample")

    all_scores, all_soft, my_unit, my_length, new_queue = call(
        functools.partial(gathered_body, factor),
        (
            shape((share, new_total)),
            pltpu.HBM((share, new_total), F32),
            shape((share, FEATURE_WIDTH)),
            shape((share, 1)),
            shape((QUEUE_PER_INDEX, FEATURE_WIDTH), BF16),
        ),
        (place, first, in_hbm(everyone), in_hbm(queue), in_hbm(prototypes), proto_scale),
        16,
        4 * share * new_total * FEATURE_WIDTH,
        [
            pltpu.VMEM(everyone.shape, BF16),
            pltpu.VMEM((share, FEATURE_WIDTH), BF16),
            pltpu.VMEM((QUEUE_PER_INDEX, FEATURE_WIDTH), BF16),
            pltpu.VMEM((share, new_total), F32),
            pltpu.VMEM((QUEUE_PER_INDEX, new_total), BF16),
            DMA((n_sample,)),
            DMA((n_sample,)),
            DMA,
            DMA,
        ],
        in_specs=[SMEM, VMEM, HBM, HBM, HBM, VMEM],
        out_specs=(VMEM, HBM, VMEM, VMEM, VMEM),
    )
    proto_grad, loss = call(
        functools.partial(gradient_body, factor),
        (shape((share, FEATURE_WIDTH)), shape((1, 1))),
        (got, all_scores, in_hbm(all_soft), in_hbm(everyone), my_unit, my_length),
        12,
        2 * share * new_total * FEATURE_WIDTH,
        [
            pltpu.VMEM((share, new_total), F32),
            pltpu.VMEM((new_total // 128, 128, FEATURE_WIDTH), BF16),
            pltpu.VMEM((share, new_total), BF16),
            DMA((4,)),
            DMA((4,)),
        ],
        in_specs=[VMEM, VMEM, HBM, HBM, VMEM, VMEM],
    )
    return (new_queue, proto_grad, loss.reshape(()))


def solution(mesh):
    split = Mesh(
        mesh.devices.reshape(8, 4, 2, mesh.shape["sample"]),
        ("proto_0", "proto_1", "proto_2", "sample"),
    )
    return jax.shard_map(
        on_device,
        mesh=split,
        in_specs=(
            P("sample", None),
            P("sample", None),
            P("sample", None),
            P(PROTO, None),
            P("sample", None),
            P("sample"),
        ),
        out_specs=(P("sample", None), P(PROTO_SAMPLE, None), P()),
        check_vma=False,
    )
```

```python
import functools
import math

import jax
import jax.numpy as jnp
from jax import lax
from jax.experimental import pallas as pl
from jax.experimental.pallas import tpu as pltpu
from jax.sharding import Mesh
from jax.sharding import PartitionSpec as P


FEATURE_WIDTH = 384
K_DEV = 2048
NEW_DEV = 256
ITERS = 3
QUEUE_PER_INDEX = 768
PROTO = ("proto_0", "proto_1", "proto_2")
PROTO_SAMPLE = ("proto_0", "proto_1", "proto_2", "sample")
ROWS = NEW_DEV + QUEUE_PER_INDEX

teacher_temp = 0.07
student_temp = 0.1
epsilon = 1e-12
TEACHER_EXP2 = math.log2(math.e) / teacher_temp
STUDENT_EXP2 = math.log2(math.e) / student_temp
F32 = jnp.float32
BF16 = jnp.bfloat16
VMEM = pl.BlockSpec(memory_space=pltpu.VMEM)
SMEM = pl.BlockSpec(memory_space=pltpu.SMEM)
HBM = pl.BlockSpec(memory_space=pltpu.HBM)
DMA = pltpu.SemaphoreType.DMA
MIB = 1024 * 1024


def call(body, out_shape, args, limit, flops, scratch=(), in_specs=None, out_specs=None):
    return pl.pallas_call(
        body,
        out_shape=out_shape,
        in_specs=in_specs or [VMEM] * len(args),
        out_specs=out_specs or jax.tree.map(lambda _: VMEM, out_shape),
        scratch_shapes=list(scratch),
        compiler_params=pltpu.CompilerParams(vmem_limit_bytes=limit * MIB),
        cost_estimate=pl.CostEstimate(flops=flops, bytes_accessed=0, transcendentals=0),
    )(*args)


def in_hbm(value):
    return pltpu.with_memory_space_constraint(value, pltpu.HBM)


def shape(dims, dtype=F32):
    return jax.ShapeDtypeStruct(dims, dtype)


def unit_rows(values):
    widened = values.astype(F32)
    length = jnp.sqrt(jnp.sum(widened * widened, axis=1, keepdims=True) + epsilon)
    return widened * (1.0 / length), length


def against(left, right):
    return lax.dot_general(left, right, (((1,), (1,)), ((), ())), preferred_element_type=F32)


def lane_sums(block):
    return jnp.sum(block.T, axis=0, keepdims=True)


def along_rows(row):
    return jnp.broadcast_to(row, (128, 128)).T


def scores_body(
    new_hbm, queue_hbm, student_hbm, owner_hbm, proto_hbm,
    scores_ref, cross_ref, message_ref, partial_ref,
    raw, hat, raw_proto, proto_hat, total, sums, owner, row_sems, proto_sems, owner_sem,
):
    def proto_copy(turn):
        rows = pl.ds(turn * 256, 256)
        return pltpu.make_async_copy(proto_hbm.at[rows], raw_proto.at[rows], proto_sems.at[turn])

    row_copies = [
        pltpu.make_async_copy(new_hbm, raw.at[pl.ds(0, NEW_DEV)], row_sems.at[0]),
        pltpu.make_async_copy(queue_hbm, raw.at[pl.ds(NEW_DEV, QUEUE_PER_INDEX)], row_sems.at[1]),
        pltpu.make_async_copy(student_hbm, raw.at[pl.ds(ROWS, NEW_DEV)], row_sems.at[2]),
    ]
    for copy in row_copies:
        copy.start()
    n_tiles = K_DEV // 256
    copies = [proto_copy(turn) for turn in range(n_tiles)]
    for copy in copies:
        copy.start()
    owner_copy = pltpu.make_async_copy(owner_hbm, owner, owner_sem)
    owner_copy.start()
    total[...] = jnp.zeros_like(total)
    sums[...] = jnp.zeros_like(sums)
    steps = [(start, min(512, ROWS - start)) for start in range(0, ROWS, 512)]

    def normalize(turn):
        span = slice(turn * 256, turn * 256 + 256)
        proto_hat[turn % 2] = unit_rows(raw_proto[span])[0].astype(BF16)

    def finish(turn):
        lanes = slice(turn * 256, turn * 256 + 256)
        proto = proto_hat[turn % 2]
        column = jnp.zeros((8, 256), F32)
        for first, length in steps:
            product = against(hat[first : first + length], proto)
            for start in range(0, length, 64):
                rows = slice(first + start, first + start + 64)
                scores = jnp.exp2(product[start : start + 64] * TEACHER_EXP2)
                scores_ref[rows, lanes] = scores
                column += jnp.sum(scores.reshape(8, 8, 256), axis=0)
        product = against(hat[ROWS:], proto)
        for start in range(0, NEW_DEV, 64):
            rows = slice(start, start + 64)
            logits = product[rows]
            cross_ref[rows, lanes] = scores_ref[rows, lanes] * (logits * (1.0 / student_temp))
            exped = jnp.exp2(logits * STUDENT_EXP2)
            total[rows] += exped[:, :128] + exped[:, 128:]
        column = jnp.sum(column, axis=0, keepdims=True)
        sums[2 * turn : 2 * turn + 1] = column[:, :128]
        sums[2 * turn + 1 : 2 * turn + 2] = column[:, 128:]

    for copy in row_copies:
        copy.wait()
    copies[0].wait()
    for start in range(0, ROWS + NEW_DEV, 64):
        rows = slice(start, start + 64)
        hat[rows] = unit_rows(raw[rows])[0].astype(BF16)
    normalize(0)
    for copy in copies[1:]:
        copy.wait()
    for turn in range(n_tiles):
        if turn + 1 < n_tiles:
            normalize(turn + 1)
        finish(turn)
    for part in range(NEW_DEV // 128):
        partial_ref[part : part + 1] = lane_sums(total[part * 128 : part * 128 + 128])
    owner_copy.wait()
    sums[K_DEV // 128 : K_DEV // 128 + 2] = owner[...].astype(F32)
    message = sums[...].astype(BF16)
    for peer in range(message_ref.shape[0]):
        message_ref[peer] = message


def received(got_ref, n_rows):
    total = got_ref[0, :n_rows].astype(F32)
    for peer in range(1, got_ref.shape[0]):
        total += got_ref[peer, :n_rows].astype(F32)
    return total


def weigh_columns(source_ref, scale_ref, block):
    total = None
    for turn in range(K_DEV // 128):
        part = source_ref[block, turn * 128 : turn * 128 + 128] * scale_ref[turn : turn + 1]
        total = part if turn == 0 else total + part
    return lane_sums(total)


def row_totals_body(factor, got_ref, scores_ref, message_ref, scale, totals):
    scale[...] = 1.0 / (received(got_ref, K_DEV // 128) * factor)
    for part in range(ROWS // 128):
        block = slice(part * 128, part * 128 + 128)
        totals[part : part + 1] = weigh_columns(scores_ref, scale, block)
    message = totals[...].astype(message_ref.dtype)
    for peer in range(message_ref.shape[0]):
        message_ref[peer] = message


def last_totals_body(
    factor, got_ref, scores_ref, cross_ref, partial_ref, message_ref, scale_ref
):
    scale_ref[...] = 1.0 / (received(got_ref, K_DEV // 128) * factor)
    rows = []
    for source in (scores_ref, cross_ref):
        for part in range(NEW_DEV // 128):
            block = slice(part * 128, part * 128 + 128)
            rows.append(weigh_columns(source, scale_ref, block))
    for part in range(NEW_DEV // 128):
        rows.append(partial_ref[part : part + 1])
    message_ref[...] = jnp.broadcast_to(jnp.concatenate(rows, axis=1)[None], message_ref.shape)


def column_sums_body(factor, got_ref, scores_ref, message_ref, weights, sums):
    scale = 1.0 / (received(got_ref, ROWS // 128) * factor)
    for part in range(ROWS // 128):
        weights[part * 128 : part * 128 + 128] = along_rows(scale[part : part + 1])
    for chunk in range(K_DEV // 128):
        lanes = slice(chunk * 128, chunk * 128 + 128)
        total = jnp.zeros((8, 128), F32)
        for start in range(0, ROWS, 64):
            rows = slice(start, start + 64)
            part = scores_ref[rows, lanes] * weights[rows]
            total += jnp.sum(part.reshape(8, 8, 128), axis=0)
        sums[chunk : chunk + 1] = jnp.sum(total, axis=0, keepdims=True)
    message = sums[...].astype(message_ref.dtype)
    for peer in range(message_ref.shape[0]):
        message_ref[peer] = message


def message_lanes(chunk):
    return chunk // 2, slice((chunk % 2) * 128, (chunk % 2) * 128 + 128)


def gathered_body(
    factor, place_ref, first_ref, student_hbm, teacher_hbm, queue_hbm, proto_hbm, scale_ref,
    scores_ref, soft_hbm, hat_hbm, unit_ref, length_ref, out_ref,
    students, teachers, proto_in, queue_in, soft, hat, chosen,
    in_sems, soft_sems, hat_sems, proto_sem, queue_sem,
):
    n_new = student_hbm.shape[0]
    share = unit_ref.shape[0]
    first = pl.multiple_of(place_ref[0] * share, share)
    n_parts = soft_sems.shape[0]
    step = n_new // n_parts
    student_copy = pltpu.make_async_copy(student_hbm, students, in_sems.at[0])
    teacher_copy = pltpu.make_async_copy(teacher_hbm, teachers, in_sems.at[1])
    proto_copy = pltpu.make_async_copy(proto_hbm.at[pl.ds(first, share)], proto_in, proto_sem)
    queue_copy = pltpu.make_async_copy(queue_hbm, queue_in, queue_sem)
    proto_copy.start()
    student_copy.start()
    teacher_copy.start()
    queue_copy.start()

    def out_copies(part):
        span = pl.ds(part * step, step)
        return (
            pltpu.make_async_copy(soft.at[:, span], soft_hbm.at[:, span], soft_sems.at[part]),
            pltpu.make_async_copy(hat.at[span], hat_hbm.at[span], hat_sems.at[part]),
        )

    columns = [
        along_rows(scale_ref[pl.ds(place_ref[0] * 2 + part, 1), :] * factor)
        for part in range(share // 128)
    ]
    proto_copy.wait()
    unit, length = unit_rows(proto_in[...])
    unit_ref[...] = unit
    length_ref[...] = length
    proto = unit.astype(BF16)
    student_copy.wait()
    for part in range(n_parts):
        for start in range(part * step, part * step + step, 128):
            rows = slice(start, start + 128)
            hat[rows] = unit_rows(students[rows])[0].astype(BF16)
            soft[:, rows] = jnp.exp2(against(proto, hat[rows]) * STUDENT_EXP2)
        for copy in out_copies(part):
            copy.start()
    teacher_copy.wait()
    for start in range(0, n_new, 128):
        rows = slice(start, start + 128)
        teacher = unit_rows(teachers[rows])[0].astype(BF16)
        scores = jnp.exp2(against(proto, teacher) * TEACHER_EXP2)
        for part in range(2):
            block = slice(part * 128, part * 128 + 128)
            scores_ref[block, rows] = scores[block] * columns[part]

    mine = place_ref[0].astype(F32)
    head = place_ref[1].astype(F32)
    size = float(QUEUE_PER_INDEX)
    earlier = lax.broadcasted_iota(jnp.int32, (128, 128), 0)
    later = lax.broadcasted_iota(jnp.int32, (128, 128), 1)
    before = jnp.where(earlier < later, 1.0, 0.0).astype(BF16)
    slots = lax.broadcasted_iota(jnp.int32, (QUEUE_PER_INDEX, 128), 0).astype(F32)
    base = jnp.zeros((1, 1), F32)
    for chunk in range(n_new // 128):
        names = first_ref[chunk // 2, K_DEV // 128 : K_DEV // 128 + 8].astype(F32)
        named = jnp.where(names[chunk % 2 : chunk % 2 + 1] == mine, 1.0, 0.0)
        ahead = jnp.dot(
            jnp.broadcast_to(named, (16, 128)).astype(BF16), before, preferred_element_type=F32
        )[:1]
        slot = head + base + ahead
        slot = jnp.where(slot >= size, slot - size, slot)
        slot = jnp.where(named > 0.5, slot, -1.0)
        chosen[:, chunk * 128 : chunk * 128 + 128] = jnp.where(slots == slot, 1.0, 0.0).astype(BF16)
        base += jnp.sum(named, axis=1, keepdims=True)
    got = jnp.dot(chosen[...], teachers[...], preferred_element_type=F32)
    turn = lax.broadcasted_iota(jnp.int32, (QUEUE_PER_INDEX, FEATURE_WIDTH), 0).astype(F32) - head
    turn = jnp.where(turn < 0.0, turn + size, turn)
    queue_copy.wait()
    out_ref[...] = jnp.where(turn < base, got, queue_in[...].astype(F32)).astype(BF16)
    for part in range(n_parts):
        for copy in out_copies(part):
            copy.wait()


def rows_body(got_ref, out_ref):
    totals = jnp.sum(got_ref[...], axis=0)
    row_scale = 1.0 / totals[:, :NEW_DEV]
    denominator = totals[:, 2 * NEW_DEV :]
    terms = jnp.log(denominator) - row_scale * totals[:, NEW_DEV : 2 * NEW_DEV]
    loss = jnp.broadcast_to(jnp.sum(terms, axis=1, keepdims=True), (1, 128))
    message = jnp.concatenate([row_scale, denominator, loss], axis=1)
    out_ref[...] = jnp.broadcast_to(message[None], out_ref.shape)


def gradient_body(
    factor, got_ref, scores_ref, soft_hbm, student_hbm, unit_ref, length_ref, out_ref, loss_ref,
    soft, student, gradient, soft_sems, student_sems,
):
    n_new = student.shape[0]
    n_parts = soft_sems.shape[0]
    step = n_new // 128 // n_parts
    soft_copies, student_copies = [], []
    for part in range(n_parts):
        span = pl.ds(part * step * 128, step * 128)
        soft_copies.append(
            pltpu.make_async_copy(soft_hbm.at[:, span], soft.at[:, span], soft_sems.at[part])
        )
        student_copies.append(
            pltpu.make_async_copy(student_hbm.at[span], student.at[span], student_sems.at[part])
        )
        soft_copies[part].start()
        student_copies[part].start()
    loss_at = 2 * NEW_DEV
    loss_ref[...] = jnp.sum(got_ref[:, :, loss_at : loss_at + 1], axis=0) * (1.0 / n_new)
    for part in range(n_parts):
        soft_copies[part].wait()
        for chunk in range(part * step, part * step + step):
            plane, names = message_lanes(chunk)
            others = slice(NEW_DEV + names.start, NEW_DEV + names.stop)
            lanes = slice(chunk * 128, chunk * 128 + 128)
            value = soft[:, lanes] * (factor / got_ref[plane, :, others])
            target = scores_ref[:, lanes] * got_ref[plane, :, names]
            gradient[:, lanes] = (value - target).astype(BF16)
    for copy in student_copies:
        copy.wait()
    unit_gradient = jnp.dot(gradient[...], student[...], preferred_element_type=F32)
    unit = unit_ref[...]
    along = jnp.sum(unit * unit_gradient, axis=1, keepdims=True)
    out_ref[...] = (unit_gradient - unit * along) / length_ref[...]


def exchange(message, axis):
    return lax.all_to_all(message, axis, split_axis=0, concat_axis=0, tiled=True)


def on_device(teacher_new, queue, student, prototypes, owners, queue_oldest_slot):
    n_sample = lax.axis_size("sample")
    n_proto = lax.axis_size(PROTO)
    protos_total = K_DEV * n_proto
    teachers_total = ROWS * n_sample
    new_total = NEW_DEV * n_sample
    share = K_DEV // n_sample
    my_index = lax.axis_index("sample")
    grad_scale = protos_total * NEW_DEV // 32
    factor = grad_scale / (new_total * student_temp)
    place = jnp.stack(
        [
            my_index.astype(jnp.int32),
            queue_oldest_slot[0].astype(jnp.int32),
        ]
    )

    all_students = lax.all_gather(student, "sample", axis=0, tiled=True)
    all_teachers = lax.all_gather(teacher_new, "sample", axis=0, tiled=True)
    scores, cross, message, partial = call(
        scores_body,
        (
            shape((ROWS, K_DEV)),
            shape((NEW_DEV, K_DEV)),
            shape((n_sample, K_DEV // 128 + 8, 128), BF16),
            shape((NEW_DEV // 128, 128)),
        ),
        (
            in_hbm(teacher_new),
            in_hbm(queue),
            in_hbm(student),
            in_hbm(owners.reshape(NEW_DEV // 128, 128)),
            in_hbm(prototypes),
        ),
        10,
        2 * (ROWS + NEW_DEV) * K_DEV * FEATURE_WIDTH,
        [
            pltpu.VMEM((ROWS + NEW_DEV, FEATURE_WIDTH), BF16),
            pltpu.VMEM((ROWS + NEW_DEV, FEATURE_WIDTH), BF16),
            pltpu.VMEM((K_DEV, FEATURE_WIDTH), BF16),
            pltpu.VMEM((2, 256, FEATURE_WIDTH), BF16),
            pltpu.VMEM((NEW_DEV, 128), F32),
            pltpu.VMEM((K_DEV // 128 + 8, 128), F32),
            pltpu.VMEM((NEW_DEV // 128, 128), jnp.int32),
            DMA((3,)),
            DMA((K_DEV // 256,)),
            DMA,
        ],
        in_specs=[HBM] * 5,
    )
    first = got = exchange(message, "sample")
    for iteration in range(ITERS - 1):
        message = call(
            functools.partial(row_totals_body, protos_total),
            shape((n_proto, ROWS // 128, 128), BF16),
            (got, scores),
            4,
            2 * ROWS * K_DEV,
            [pltpu.VMEM((K_DEV // 128, 128), F32), pltpu.VMEM((ROWS // 128, 128), F32)],
        )
        got = exchange(message, PROTO)
        wide = iteration == ITERS - 2
        message = call(
            functools.partial(column_sums_body, teachers_total),
            shape((n_sample, K_DEV // 128, 128), F32 if wide else BF16),
            (got, scores),
            4,
            2 * ROWS * K_DEV,
            [pltpu.VMEM((ROWS, 128), F32), pltpu.VMEM((K_DEV // 128, 128), F32)],
        )
        got = exchange(message, "sample")

    message, proto_scale = call(
        functools.partial(last_totals_body, protos_total),
        (shape((n_proto, 1, 3 * NEW_DEV)), shape((K_DEV // 128, 128))),
        (got, scores, cross, partial),
        4,
        4 * NEW_DEV * K_DEV,
    )
    got = exchange(message, PROTO)
    message = call(
        rows_body, shape((n_sample, 1, 2 * NEW_DEV + 128)), (got,), 4, n_proto * 3 * NEW_DEV
    )
    got = exchange(message, "sample")

    all_scores, all_soft, all_hats, my_unit, my_length, new_queue = call(
        functools.partial(gathered_body, factor),
        (
            shape((share, new_total)),
            pltpu.HBM((share, new_total), F32),
            pltpu.HBM((new_total, FEATURE_WIDTH), BF16),
            shape((share, FEATURE_WIDTH)),
            shape((share, 1)),
            shape((QUEUE_PER_INDEX, FEATURE_WIDTH), BF16),
        ),
        (
            place,
            first,
            in_hbm(all_students),
            in_hbm(all_teachers),
            in_hbm(queue),
            in_hbm(prototypes),
            proto_scale,
        ),
        16,
        4 * share * new_total * FEATURE_WIDTH,
        [
            pltpu.VMEM((new_total, FEATURE_WIDTH), BF16),
            pltpu.VMEM((new_total, FEATURE_WIDTH), BF16),
            pltpu.VMEM((share, FEATURE_WIDTH), BF16),
            pltpu.VMEM((QUEUE_PER_INDEX, FEATURE_WIDTH), BF16),
            pltpu.VMEM((share, new_total), F32),
            pltpu.VMEM((new_total, FEATURE_WIDTH), BF16),
            pltpu.VMEM((QUEUE_PER_INDEX, new_total), BF16),
            DMA((2,)),
            DMA((4,)),
            DMA((4,)),
            DMA,
            DMA,
        ],
        in_specs=[SMEM, VMEM, HBM, HBM, HBM, HBM, VMEM],
        out_specs=(VMEM, HBM, HBM, VMEM, VMEM, VMEM),
    )
    proto_grad, loss = call(
        functools.partial(gradient_body, factor),
        (shape((share, FEATURE_WIDTH)), shape((1, 1))),
        (got, all_scores, in_hbm(all_soft), in_hbm(all_hats), my_unit, my_length),
        12,
        2 * share * new_total * FEATURE_WIDTH,
        [
            pltpu.VMEM((share, new_total), F32),
            pltpu.VMEM((new_total, FEATURE_WIDTH), BF16),
            pltpu.VMEM((share, new_total), BF16),
            DMA((4,)),
            DMA((4,)),
        ],
        in_specs=[VMEM, VMEM, HBM, HBM, VMEM, VMEM],
    )
    return (new_queue, proto_grad, loss.reshape(()))


def solution(mesh):
    split = Mesh(
        mesh.devices.reshape(8, 4, 2, mesh.shape["sample"]),
        ("proto_0", "proto_1", "proto_2", "sample"),
    )
    return jax.shard_map(
        on_device,
        mesh=split,
        in_specs=(
            P("sample", None),
            P("sample", None),
            P("sample", None),
            P(PROTO, None),
            P("sample", None),
            P("sample"),
        ),
        out_specs=(P("sample", None), P(PROTO_SAMPLE, None), P()),
        check_vma=False,
    )
```
